128 devices in a mesh: band: 4 (over y_lo, core), grid: 32 (over x, z, y_hi).
Axes of the slice: x: 4, y: 4 (y_hi: 2, y_lo: 2; y = y_hi * 2 + y_lo), z: 4, core: 2. Of those that a mesh axis runs over, the one named last changes fastest.
Arguments:
- orbitals: bfloat16 [64, 2, 64, 128, 128], P('band', None, 'grid'), may hold values from -1.5 to 1.5
- occupations: float32 [64], P('band'), may hold values from 0.2 to 2
Outputs:
- current: float32 [3, 64, 128, 128], P(None, 'grid', 'band')
The draws below stay inside these ranges and needn't reach their ends.
All inputs are finite; a program needn't handle non-finite values.
Results may differ from the reference program's by a relative error of at most 0.0003.
Values may be sent and summed in bfloat16 or wider, within the bound.
A program may use at most 64 MiB of HBM per device.

```python
import jax
import jax.numpy as jnp
from jax import lax

NX = 128
NY = 128
BANDS = 64
NZ = 64


def block_scale(key, extent, cuts, smallest, top_value):
    def one(axis_at, parts):
        steps = jax.random.uniform(jax.random.fold_in(jax.random.fold_in(key, 6), axis_at), (parts,), jnp.float32, smallest / len(cuts), top_value / len(cuts))
        return jnp.repeat(jnp.exp(steps), extent[axis_at] // parts).reshape((-1,) + (1,) * (len(extent) - axis_at - 1))

    level = one(*cuts[0])
    for cut in cuts[1:]:
        level = level * one(*cut)
    return level


def normal_values(key, shape, width, reach, pieces=(), held_as=jnp.bfloat16):
    entries = width * jax.random.normal(key, shape, jnp.float32)
    if pieces:
        entries = entries * block_scale(key, shape, pieces, -0.22, 0.18)
    return jnp.clip(entries, -reach, reach).astype(held_as)


def setup_inputs(seed: int = 0) -> dict:
    splits = jax.random.split(jax.random.key(seed), 3)
    return {
        "orbitals": normal_values(splits[0], (BANDS, 2, NZ, NX, NY), 0.25, 1.5, ((0, 4), (2, 32))),
        "occupations": jnp.clip(0.2 + 1.8 * jax.random.uniform(splits[1], (BANDS,), jnp.float32) ** block_scale(splits[1], (BANDS,), ((0, 4),), -0.2, 0.2), 0.2, 2.0),
    }


def derivative(values, direction):
    forward = jnp.roll(values, -1, direction) - jnp.roll(values, 1, direction)
    farther = jnp.roll(values, -2, direction) - jnp.roll(values, 2, direction)
    return (8.0 * forward - farther) / 12.0


def reference(orbitals, occupations):
    def advance(summed, item):
        orbital, weight = item
        real_part = orbital[0].astype(jnp.float32)
        imag_part = orbital[1].astype(jnp.float32)
        components = jnp.stack([real_part * derivative(imag_part, direction) - imag_part * derivative(real_part, direction) for direction in range(3)])
        return summed + weight * components, None

    initial = jnp.zeros((3, NZ, NX, NY), jnp.float32)
    summed, _ = lax.scan(advance, initial, (orbitals, occupations))
    return summed
```

```python
import jax
import jax.numpy as jnp
from jax import lax
from jax.experimental import pallas as pl
from jax.experimental.pallas import tpu as pltpu
from jax.sharding import PartitionSpec as P

MESH = pl.DeviceIdType.MESH
F32 = jnp.float32
BF16 = jnp.bfloat16


def stencil(n, transposed):
    i = lax.broadcasted_iota(jnp.int32, (n, n), 0)
    j = lax.broadcasted_iota(jnp.int32, (n, n), 1)
    d = (i - j if transposed else j - i) + n
    d = jnp.where(d >= n, d - n, d)
    near = jnp.where(d == 1, 8.0, 0.0) - jnp.where(d == n - 1, 8.0, 0.0)
    far = jnp.where(d == n - 2, 1.0, 0.0) - jnp.where(d == 2, 1.0, 0.0)
    return (near + far).astype(BF16)


def make_kernel(rings):
    def kernel(
        orb, occ, out,
        own, outer, inner, below, above, weights, mat_x, mat_y,
        x_acc, x_in, y_acc, pairs, main_out, main_in, extra_out, extra_in,
        load_sem, outer_send, outer_recv, inner_send, inner_recv, down_send, down_recv, up_send, up_recv,
        weight_send, weight_recv, x_send, x_recv, main_send, main_recv, extra_send, extra_recv,
    ):
        bands = own.shape[0]
        b = lax.axis_index("band")
        g = lax.axis_index("grid")
        ring, s = g // 2, g % 2
        yl, c = b // 2, b % 2
        me = s * 4 + b

        def device(r, s_, yl_, c_):
            return {"band": 2 * yl_ + c_, "grid": 2 * ((r + rings) % rings) + s_}

        load = pltpu.make_async_copy(orb, own, load_sem)
        load.start()

        flips = [(1, 0, 0), (1, 0, 1), (0, 1, 0), (1, 1, 0), (0, 1, 1), (1, 1, 1), (0, 0, 1)]
        peers = [((s + i) % 2, (yl + j) % 2, (c + k) % 2) for i, j, k in flips]
        yo = 1 - yl
        barrier = pltpu.get_barrier_semaphore()

        def greet(target):
            pl.semaphore_signal(barrier, inc=1, device_id=target, device_id_type=MESH)

        for s_, yl_, c_ in peers:
            greet(device(ring, s_, yl_, c_))
        greet(device(ring + 1, s, yl, c))
        greet(device(ring - 1, s, yl, c))
        back = ring + 2 * s - 1
        greet(device(back, 0, yo, c))
        greet(device(back, 1, yo, c))

        for n in range(bands):
            weights[b, n : n + 1, :] = jnp.full((1, 128), occ[n], F32)
        mat_x[...] = stencil(128, False)
        mat_y[...] = stencil(128, True)
        x_acc[...] = jnp.zeros_like(x_acc)
        y_acc[...] = jnp.zeros_like(y_acc)
        load.wait()
        pl.semaphore_wait(barrier, 11)

        def send(src, dst, ssem, rsem, target):
            copy = pltpu.make_async_remote_copy(
                src_ref=src, dst_ref=dst, send_sem=ssem, recv_sem=rsem, device_id=target, device_id_type=MESH
            )
            copy.start()
            return copy

        sent = []

        def exchange(plane, slots, ssem, rsem):
            for k, (s_, yl_, c_) in enumerate(peers):
                row = pl.multiple_of(32 * (2 * (1 - yl_) + c_) + 16 * s_, 16)
                sent.append(
                    send(
                        own.at[:, :, plane, pl.ds(row, 16), :], slots.at[me], ssem.at[k], rsem.at[me],
                        device(ring, s_, yl_, c_),
                    )
                )
            row = pl.multiple_of(32 * (2 * yo + c) + 16 * s, 16)
            pltpu.make_async_copy(orb.at[:, :, plane, pl.ds(row, 16), :], slots.at[me], rsem.at[me]).start()

        exchange(s, outer, outer_send, outer_recv)
        for k, (j, i) in enumerate([(0, 1), (1, 0), (1, 1)]):
            sent.append(
                send(
                    weights.at[b], weights.at[b], weight_send.at[k], weight_recv.at[b],
                    device(ring, s, (yl + j) % 2, (c + i) % 2),
                )
            )

        def x_step(n, _):
            w = occ[n]
            for z in range(2):
                re = own[n, 0, z]
                im = own[n, 1, z]
                dre = jnp.dot(mat_x[...], re, preferred_element_type=F32)
                dim = jnp.dot(mat_x[...], im, preferred_element_type=F32)
                x_acc[z] += w * (re.astype(F32) * dim - im.astype(F32) * dre)
            return 0

        lax.fori_loop(0, bands, x_step, 0)

        exchange(1 - s, inner, inner_send, inner_recv)
        for j in range(1, 4):
            to = (b + j) % 4
            sent.append(
                send(
                    x_acc.at[:, pl.ds(pl.multiple_of(32 * to, 32), 32), :], x_in.at[b],
                    x_send.at[j - 1], x_recv.at[b], device(ring, s, to // 2, to % 2),
                )
            )

        def arrived(ref, sem):
            pltpu.make_async_copy(ref, ref, sem).wait()

        for j in range(1, 4):
            q = (b + j) % 4
            arrived(weights.at[q], weight_recv.at[q])

        def y_current(slots, k, q, plane):
            def step(m, total):
                n = 4 * m
                block = slots[k, pl.ds(n, 4)]
                grad = jnp.dot(block.reshape(128, 128), mat_y[...], preferred_element_type=F32).reshape(4, 2, 16, 128)
                for i in range(4):
                    w = weights[q, pl.ds(n + i, 1), :]
                    re = block[i, 0].astype(F32)
                    im = block[i, 1].astype(F32)
                    total = total + w * (re * grad[i, 1] - im * grad[i, 0])
                return total

            y_acc[plane] = lax.fori_loop(0, bands // 4, step, y_acc[plane])

        for j, i in [(0, 0), (0, 1), (1, 0), (1, 1)]:
            q = 2 * ((yl + j) % 2) + (c + i) % 2
            for s_ in range(2):
                k = 4 * s_ + q
                arrived(outer.at[k], outer_recv.at[k])
                if s_ == 0:
                    sent.append(send(outer.at[k], above.at[q], down_send.at[q], down_recv.at[q], device(ring - 1, s, yl, c)))
                else:
                    sent.append(send(outer.at[k], below.at[q], up_send.at[q], up_recv.at[q], device(ring + 1, s, yl, c)))
                y_current(outer, k, q, 3 * s_)

        pairs[...] = jnp.zeros_like(pairs)
        for j, i in [(0, 0), (0, 1), (1, 0), (1, 1)]:
            q = 2 * ((yl + j) % 2) + (c + i) % 2
            arrived(above.at[q], down_recv.at[q])
            arrived(below.at[q], up_recv.at[q])
            arrived(inner.at[q], inner_recv.at[q])
            arrived(inner.at[4 + q], inner_recv.at[4 + q])

            def z_step(n, sums):
                w = weights[q, pl.ds(n, 1), :]

                def field(slots, k):
                    return slots[k, n, 0].astype(F32), slots[k, n, 1].astype(F32)

                def term(u, v):
                    return u[0] * v[1] - u[1] * v[0]

                def weighted(u):
                    return w * u[0], w * u[1]

                a0, b1 = field(outer, q), field(outer, 4 + q)
                a1, b0 = field(inner, q), field(inner, 4 + q)
                nxt, prv = field(above, q), field(below, q)
                wa1, wb0, wn = weighted(a1), weighted(b0), weighted(nxt)
                terms = (
                    term(a0, wa1), term(wa1, b0), term(wb0, b1), term(a0, wb0), term(wa1, b1),
                    term(b1, wn), term(b0, wn), term(prv, wa1),
                )
                return tuple(x + t for x, t in zip(sums, terms))

            sums = lax.fori_loop(0, bands, z_step, tuple(pairs[p] for p in range(8)))
            for p in range(8):
                pairs[p] = sums[p]
            y_current(inner, q, q, 1)
            y_current(inner, 4 + q, q, 2)

        a01, a1b0, b01, a0b0, a1b1, b1n0, b0n0, p1a1 = (pairs[p] for p in range(8))
        near, far = 8.0 / 12.0, 1.0 / 12.0
        extra_out[0] = near * b1n0 - far * b0n0
        extra_out[1] = -far * p1a1
        main_out[0, 0, 0] = near * a01 - far * a0b0
        main_out[0, 0, 1] = near * (a1b0 + a01) - far * (a1b1 + p1a1)
        main_out[1, 0, 0] = near * (b01 + a1b0) - far * (b0n0 + a0b0)
        main_out[1, 0, 1] = near * (b1n0 + b01) - far * a1b1
        for p in range(4):
            main_out[p // 2, 1, p % 2] = y_acc[p] * (1.0 / 12.0)
        for e, r in ((0, ring + 1), (1, ring - 1)):
            sent.append(send(extra_out.at[e], extra_in.at[s], extra_send.at[e], extra_recv.at[s], device(r, e, yo, c)))
        for e in range(2):
            sent.append(send(main_out.at[e], main_in.at[s], main_send.at[e], main_recv.at[s], device(ring, e, yo, c)))

        total = x_acc[:, pl.ds(pl.multiple_of(32 * b, 32), 32), :]
        for j in range(1, 4):
            q = (b + j) % 4
            arrived(x_in.at[q], x_recv.at[q])
            total = total + x_in[q]
        out[1] = total * (1.0 / 12.0)
        for h in range(2):
            rows = slice(16 * h, 16 * h + 16)
            arrived(main_in.at[h], main_recv.at[h])
            arrived(extra_in.at[h], extra_recv.at[h])
            out[0, :, rows, :] = main_in[h, 0]
            out[2, :, rows, :] = main_in[h, 1]
            out[0, s, rows, :] += extra_in[h]
        for copy in sent:
            copy.wait_send()

    return kernel


def solution(mesh):
    rings = mesh.shape["grid"] // 2

    def per_device(orbitals, occupations):
        n = orbitals.shape[0]
        dma = pltpu.SemaphoreType.DMA
        chunk = (n, 2, 16, 128)
        return pl.pallas_call(
            make_kernel(rings),
            out_shape=jax.ShapeDtypeStruct((3, 2, 32, 128), F32),
            in_specs=[pl.BlockSpec(memory_space=pl.ANY), pl.BlockSpec(memory_space=pltpu.SMEM)],
            out_specs=pl.BlockSpec(memory_space=pltpu.VMEM),
            scratch_shapes=[
                pltpu.VMEM((n, 2, 2, 128, 128), BF16),
                pltpu.VMEM((8, *chunk), BF16),
                pltpu.VMEM((8, *chunk), BF16),
                pltpu.VMEM((4, *chunk), BF16),
                pltpu.VMEM((4, *chunk), BF16),
                pltpu.VMEM((4, n, 128), F32),
                pltpu.VMEM((128, 128), BF16),
                pltpu.VMEM((128, 128), BF16),
                pltpu.VMEM((2, 128, 128), F32),
                pltpu.VMEM((4, 2, 32, 128), F32),
                pltpu.VMEM((4, 16, 128), F32),
                pltpu.VMEM((8, 16, 128), F32),
                pltpu.VMEM((2, 2, 2, 16, 128), F32),
                pltpu.VMEM((2, 2, 2, 16, 128), F32),
                pltpu.VMEM((2, 16, 128), F32),
                pltpu.VMEM((2, 16, 128), F32),
                dma,
                dma((7,)), dma((8,)),
                dma((7,)), dma((8,)),
                dma((4,)), dma((4,)),
                dma((4,)), dma((4,)),
                dma((3,)), dma((4,)),
                dma((3,)), dma((4,)),
                dma((2,)), dma((2,)),
                dma((2,)), dma((2,)),
            ],
            compiler_params=pltpu.CompilerParams(collective_id=0, has_side_effects=True),
        )(orbitals, occupations)

    return jax.shard_map(
        per_device,
        mesh=mesh,
        in_specs=(P("band", None, "grid", None, None), P("band")),
        out_specs=P(None, "grid", "band", None),
        check_vma=False,
    )
```

```python
import jax
import jax.numpy as jnp
from jax import lax
from jax.experimental import pallas as pl
from jax.experimental.pallas import tpu as pltpu
from jax.sharding import PartitionSpec as P

MESH = pl.DeviceIdType.MESH
F32 = jnp.float32
BF16 = jnp.bfloat16


def stencil(n, transposed):
    i = lax.broadcasted_iota(jnp.int32, (n, n), 0)
    j = lax.broadcasted_iota(jnp.int32, (n, n), 1)
    d = (i - j if transposed else j - i) + n
    d = jnp.where(d >= n, d - n, d)
    near = jnp.where(d == 1, 8.0, 0.0) - jnp.where(d == n - 1, 8.0, 0.0)
    far = jnp.where(d == n - 2, 1.0, 0.0) - jnp.where(d == 2, 1.0, 0.0)
    return (near + far).astype(BF16)


def make_kernel(rings):
    def kernel(
        orb, occ_in, out,
        occ, own, outer, inner, below, above, weights, mat_x, mat_y,
        x_acc, x_in, y_acc, pairs, main_out, main_in, extra_out, extra_in,
        occ_sem, load_sem, outer_send, outer_recv, inner_send, inner_recv, down_send, down_recv, up_send, up_recv,
        weight_send, weight_recv, x_send, x_recv, main_send, main_recv, extra_send, extra_recv,
    ):
        bands = own.shape[0]
        b = lax.axis_index("band")
        g = lax.axis_index("grid")
        ring, s = g // 2, g % 2
        yl, c = b // 2, b % 2
        me = s * 4 + b

        def device(r, s_, yl_, c_):
            return {"band": 2 * yl_ + c_, "grid": 2 * ((r + rings) % rings) + s_}

        flips = [(0, 0, 1), (1, 0, 0), (1, 0, 1), (0, 1, 0), (1, 1, 0), (0, 1, 1), (1, 1, 1)]
        peers = [((s + i) % 2, (yl + j) % 2, (c + k) % 2) for i, j, k in flips]
        yo = 1 - yl
        barrier = pltpu.get_barrier_semaphore()

        def greet(target):
            pl.semaphore_signal(barrier, inc=1, device_id=target, device_id_type=MESH)

        for s_, yl_, c_ in peers:
            greet(device(ring, s_, yl_, c_))
        greet(device(ring + 1, s, yl, c))
        greet(device(ring - 1, s, yl, c))
        back = ring + 2 * s - 1
        greet(device(back, 0, yo, c))
        greet(device(back, 1, yo, c))

        occ_load = pltpu.make_async_copy(occ_in, occ, occ_sem)
        occ_load.start()
        loads = [
            pltpu.make_async_copy(orb.at[:, :, plane], own.at[:, :, plane], load_sem.at[k])
            for k, plane in enumerate((s, 1 - s))
        ]
        for load in loads:
            load.start()
        my_row = pl.multiple_of(32 * (2 * yo + c) + 16 * s, 16)
        for plane, slots, sem in ((s, outer, outer_recv), (1 - s, inner, inner_recv)):
            pltpu.make_async_copy(orb.at[:, :, plane, pl.ds(my_row, 16), :], slots.at[me], sem.at[me]).start()
        mat_x[...] = stencil(128, False)
        mat_y[...] = stencil(128, True)
        x_acc[...] = jnp.zeros_like(x_acc)
        y_acc[...] = jnp.zeros_like(y_acc)
        pairs[...] = jnp.zeros_like(pairs)

        occ_load.wait()
        for n in range(bands):
            weights[b, n : n + 1, :] = jnp.full((1, 128), occ[n], F32)
        loads[0].wait()
        pl.semaphore_wait(barrier, 11)

        def send(src, dst, ssem, rsem, target):
            copy = pltpu.make_async_remote_copy(
                src_ref=src, dst_ref=dst, send_sem=ssem, recv_sem=rsem, device_id=target, device_id_type=MESH
            )
            copy.start()
            return copy

        sent = []

        def exchange(plane, slots, ssem, rsem):
            for k, (s_, yl_, c_) in enumerate(peers):
                row = pl.multiple_of(32 * (2 * (1 - yl_) + c_) + 16 * s_, 16)
                sent.append(
                    send(
                        own.at[:, :, plane, pl.ds(row, 16), :], slots.at[me], ssem.at[k], rsem.at[me],
                        device(ring, s_, yl_, c_),
                    )
                )

        for k, (j, i) in enumerate([(0, 1), (1, 0), (1, 1)]):
            sent.append(
                send(
                    weights.at[b], weights.at[b], weight_send.at[k], weight_recv.at[b],
                    device(ring, s, (yl + j) % 2, (c + i) % 2),
                )
            )

        exchange(s, outer, outer_send, outer_recv)
        loads[1].wait()

        def x_step(n, _):
            w = occ[n]
            for z in range(2):
                re = own[n, 0, z]
                im = own[n, 1, z]
                dre = jnp.dot(mat_x[...], re, preferred_element_type=F32)
                dim = jnp.dot(mat_x[...], im, preferred_element_type=F32)
                x_acc[z] += w * (re.astype(F32) * dim - im.astype(F32) * dre)
            return 0

        lax.fori_loop(0, bands, x_step, 0)

        exchange(1 - s, inner, inner_send, inner_recv)
        for j in range(1, 4):
            to = (b + j) % 4
            sent.append(
                send(
                    x_acc.at[:, pl.ds(pl.multiple_of(32 * to, 32), 32), :], x_in.at[b],
                    x_send.at[j - 1], x_recv.at[b], device(ring, s, to // 2, to % 2),
                )
            )

        def arrived(ref, sem):
            pltpu.make_async_copy(ref, ref, sem).wait()

        def y_current(slots, k, q, plane):
            block = slots[k]
            grad = jnp.dot(block.reshape(bands * 32, 128), mat_y[...], preferred_element_type=F32)
            total = y_acc[plane]
            for n in range(bands):
                re, im = block[n, 0].astype(F32), block[n, 1].astype(F32)
                dre, dim = grad[32 * n : 32 * n + 16], grad[32 * n + 16 : 32 * n + 32]
                total = total + weights[q, n : n + 1, :] * (re * dim - im * dre)
            y_acc[plane] = total

        for j, i in [(0, 0), (0, 1), (1, 0), (1, 1)]:
            q = 2 * ((yl + j) % 2) + (c + i) % 2
            for s_ in range(2):
                k = 4 * s_ + q
                arrived(outer.at[k], outer_recv.at[k])
                if s_ == 0:
                    sent.append(send(outer.at[k], above.at[q], down_send.at[q], down_recv.at[q], device(ring - 1, s, yl, c)))
                else:
                    sent.append(send(outer.at[k], below.at[q], up_send.at[q], up_recv.at[q], device(ring + 1, s, yl, c)))
            if j + i > 0:
                arrived(weights.at[q], weight_recv.at[q])
            for s_ in range(2):
                k = 4 * s_ + q
                y_current(outer, k, q, 3 * s_)

        for j, i in [(0, 0), (0, 1), (1, 0), (1, 1)]:
            q = 2 * ((yl + j) % 2) + (c + i) % 2
            arrived(above.at[q], down_recv.at[q])
            arrived(below.at[q], up_recv.at[q])
            arrived(inner.at[q], inner_recv.at[q])
            arrived(inner.at[4 + q], inner_recv.at[4 + q])

            def z_step(n, sums):
                w = weights[q, pl.ds(n, 1), :]

                def field(slots, k):
                    return slots[k, n, 0].astype(F32), slots[k, n, 1].astype(F32)

                def term(u, v):
                    return u[0] * v[1] - u[1] * v[0]

                def weighted(u):
                    return w * u[0], w * u[1]

                a0, b1 = field(outer, q), field(outer, 4 + q)
                a1, b0 = field(inner, q), field(inner, 4 + q)
                nxt, prv = field(above, q), field(below, q)
                wa1, wb0, wn = weighted(a1), weighted(b0), weighted(nxt)
                terms = (
                    term(a0, wa1), term(wa1, b0), term(wb0, b1), term(a0, wb0), term(wa1, b1),
                    term(b1, wn), term(b0, wn), term(prv, wa1),
                )
                return tuple(x + t for x, t in zip(sums, terms))

            sums = lax.fori_loop(0, bands, z_step, tuple(pairs[p] for p in range(8)))
            for p in range(8):
                pairs[p] = sums[p]
            y_current(inner, q, q, 1)
            y_current(inner, 4 + q, q, 2)

        a01, a1b0, b01, a0b0, a1b1, b1n0, b0n0, p1a1 = (pairs[p] for p in range(8))
        near, far = 8.0 / 12.0, 1.0 / 12.0
        extra_out[0] = near * b1n0 - far * b0n0
        extra_out[1] = -far * p1a1
        main_out[0, 0, 0] = near * a01 - far * a0b0
        main_out[0, 0, 1] = near * (a1b0 + a01) - far * (a1b1 + p1a1)
        main_out[1, 0, 0] = near * (b01 + a1b0) - far * (b0n0 + a0b0)
        main_out[1, 0, 1] = near * (b1n0 + b01) - far * a1b1
        for p in range(4):
            main_out[p // 2, 1, p % 2] = y_acc[p] * (1.0 / 12.0)
        for e, r in ((0, ring + 1), (1, ring - 1)):
            sent.append(send(extra_out.at[e], extra_in.at[s], extra_send.at[e], extra_recv.at[s], device(r, e, yo, c)))
        for e in range(2):
            sent.append(send(main_out.at[e], main_in.at[s], main_send.at[e], main_recv.at[s], device(ring, e, yo, c)))

        total = x_acc[:, pl.ds(pl.multiple_of(32 * b, 32), 32), :]
        for j in range(1, 4):
            q = (b + j) % 4
            arrived(x_in.at[q], x_recv.at[q])
            total = total + x_in[q]
        out[1] = total * (1.0 / 12.0)
        for h in range(2):
            rows = slice(16 * h, 16 * h + 16)
            arrived(main_in.at[h], main_recv.at[h])
            arrived(extra_in.at[h], extra_recv.at[h])
            out[0, :, rows, :] = main_in[h, 0]
            out[2, :, rows, :] = main_in[h, 1]
            out[0, s, rows, :] += extra_in[h]
        for copy in sent:
            copy.wait_send()

    return kernel


def solution(mesh):
    rings = mesh.shape["grid"] // 2

    def per_device(orbitals, occupations):
        n = orbitals.shape[0]
        dma = pltpu.SemaphoreType.DMA
        chunk = (n, 2, 16, 128)
        return pl.pallas_call(
            make_kernel(rings),
            out_shape=jax.ShapeDtypeStruct((3, 2, 32, 128), F32),
            in_specs=[pl.BlockSpec(memory_space=pl.ANY), pl.BlockSpec(memory_space=pl.ANY)],
            out_specs=pl.BlockSpec(memory_space=pltpu.VMEM),
            scratch_shapes=[
                pltpu.SMEM((n,), F32),
                pltpu.VMEM((n, 2, 2, 128, 128), BF16),
                pltpu.VMEM((8, *chunk), BF16),
                pltpu.VMEM((8, *chunk), BF16),
                pltpu.VMEM((4, *chunk), BF16),
                pltpu.VMEM((4, *chunk), BF16),
                pltpu.VMEM((4, n, 128), F32),
                pltpu.VMEM((128, 128), BF16),
                pltpu.VMEM((128, 128), BF16),
                pltpu.VMEM((2, 128, 128), F32),
                pltpu.VMEM((4, 2, 32, 128), F32),
                pltpu.VMEM((4, 16, 128), F32),
                pltpu.VMEM((8, 16, 128), F32),
                pltpu.VMEM((2, 2, 2, 16, 128), F32),
                pltpu.VMEM((2, 2, 2, 16, 128), F32),
                pltpu.VMEM((2, 16, 128), F32),
                pltpu.VMEM((2, 16, 128), F32),
                dma,
                dma((2,)),
                dma((7,)), dma((8,)),
                dma((7,)), dma((8,)),
                dma((4,)), dma((4,)),
                dma((4,)), dma((4,)),
                dma((3,)), dma((4,)),
                dma((3,)), dma((4,)),
                dma((2,)), dma((2,)),
                dma((2,)), dma((2,)),
            ],
            compiler_params=pltpu.CompilerParams(collective_id=0, has_side_effects=True),
        )(orbitals, occupations)

    return jax.shard_map(
        per_device,
        mesh=mesh,
        in_specs=(P("band", None, "grid", None, None), P("band")),
        out_specs=P(None, "grid", "band", None),
        check_vma=False,
    )
```

```python
import jax
import jax.numpy as jnp
from jax import lax
from jax.experimental import pallas as pl
from jax.experimental.pallas import tpu as pltpu
from jax.sharding import PartitionSpec as P

MESH = pl.DeviceIdType.MESH
F32 = jnp.float32
BF16 = jnp.bfloat16


def stencil(n, transposed):
    i = lax.broadcasted_iota(jnp.int32, (n, n), 0)
    j = lax.broadcasted_iota(jnp.int32, (n, n), 1)
    d = (i - j if transposed else j - i) + n
    d = jnp.where(d >= n, d - n, d)
    near = jnp.where(d == 1, 8.0, 0.0) - jnp.where(d == n - 1, 8.0, 0.0)
    far = jnp.where(d == n - 2, 1.0, 0.0) - jnp.where(d == 2, 1.0, 0.0)
    return (near + far).astype(BF16)


def make_kernel(rings):
    def kernel(
        orb, occ_in, out,
        occ, own, outer, inner, below, above, weights, mat_x, mat_y,
        x_acc, x_in, y_acc, pairs, main_out, main_in, extra_out, extra_in,
        occ_sem, load_sem, outer_send, outer_recv, inner_send, inner_recv, down_send, down_recv, up_send, up_recv,
        weight_send, weight_recv, x_send, x_recv, main_send, main_recv, extra_send, extra_recv,
    ):
        bands = own.shape[0]
        b = lax.axis_index("band")
        g = lax.axis_index("grid")
        ring, s = g // 2, g % 2
        yl, c = b // 2, b % 2
        me = s * 4 + b

        def device(r, s_, yl_, c_):
            return {"band": 2 * yl_ + c_, "grid": 2 * ((r + rings) % rings) + s_}

        flips = [(0, 0, 1), (1, 0, 0), (1, 0, 1), (0, 1, 0), (1, 1, 0), (0, 1, 1), (1, 1, 1)]
        peers = [((s + i) % 2, (yl + j) % 2, (c + k) % 2) for i, j, k in flips]
        yo = 1 - yl
        barrier = pltpu.get_barrier_semaphore()

        def greet(target):
            pl.semaphore_signal(barrier, inc=1, device_id=target, device_id_type=MESH)

        for s_, yl_, c_ in peers:
            greet(device(ring, s_, yl_, c_))
        greet(device(ring + 1, s, yl, c))
        greet(device(ring - 1, s, yl, c))
        back = ring + 2 * s - 1
        greet(device(back, 0, yo, c))
        greet(device(back, 1, yo, c))

        occ_load = pltpu.make_async_copy(occ_in, occ, occ_sem)
        occ_load.start()
        loads = [
            pltpu.make_async_copy(orb.at[:, :, plane], own.at[:, :, plane], load_sem.at[k])
            for k, plane in enumerate((s, 1 - s))
        ]
        for load in loads:
            load.start()
        my_row = pl.multiple_of(32 * (2 * yo + c) + 16 * s, 16)
        for plane, slots, sem in ((s, outer, outer_recv), (1 - s, inner, inner_recv)):
            pltpu.make_async_copy(orb.at[:, :, plane, pl.ds(my_row, 16), :], slots.at[me], sem.at[me]).start()
        mat_x[...] = stencil(128, False)
        mat_y[...] = stencil(128, True)
        x_acc[...] = jnp.zeros_like(x_acc)
        y_acc[...] = jnp.zeros_like(y_acc)
        pairs[...] = jnp.zeros_like(pairs)

        occ_load.wait()
        for n in range(bands):
            weights[b, n : n + 1, :] = jnp.full((1, 128), occ[n], F32)
        loads[0].wait()
        pl.semaphore_wait(barrier, 11)

        def send(src, dst, ssem, rsem, target):
            copy = pltpu.make_async_remote_copy(
                src_ref=src, dst_ref=dst, send_sem=ssem, recv_sem=rsem, device_id=target, device_id_type=MESH
            )
            copy.start()
            return copy

        sent = []

        def exchange(plane, slots, ssem, rsem):
            for k, (s_, yl_, c_) in enumerate(peers):
                row = pl.multiple_of(32 * (2 * (1 - yl_) + c_) + 16 * s_, 16)
                sent.append(
                    send(
                        own.at[:, :, plane, pl.ds(row, 16), :], slots.at[me], ssem.at[k], rsem.at[me],
                        device(ring, s_, yl_, c_),
                    )
                )

        for k, (j, i) in enumerate([(0, 1), (1, 0), (1, 1)]):
            sent.append(
                send(
                    weights.at[b], weights.at[b], weight_send.at[k], weight_recv.at[b],
                    device(ring, s, (yl + j) % 2, (c + i) % 2),
                )
            )

        exchange(s, outer, outer_send, outer_recv)
        loads[1].wait()

        def x_step(n, _):
            w = occ[n]
            for z in range(2):
                re = own[n, 0, z]
                im = own[n, 1, z]
                dre = jnp.dot(mat_x[...], re, preferred_element_type=F32)
                dim = jnp.dot(mat_x[...], im, preferred_element_type=F32)
                x_acc[z] += w * (re.astype(F32) * dim - im.astype(F32) * dre)
            return 0

        lax.fori_loop(0, bands, x_step, 0)

        exchange(1 - s, inner, inner_send, inner_recv)
        for j in range(1, 4):
            to = (b + j) % 4
            sent.append(
                send(
                    x_acc.at[:, pl.ds(pl.multiple_of(32 * to, 32), 32), :], x_in.at[b],
                    x_send.at[j - 1], x_recv.at[b], device(ring, s, to // 2, to % 2),
                )
            )

        def arrived(ref, sem):
            pltpu.make_async_copy(ref, ref, sem).wait()

        def y_current(slots, k, q, plane):
            block = slots[k]
            grad = jnp.dot(block.reshape(bands * 32, 128), mat_y[...], preferred_element_type=F32)
            total = y_acc[plane]
            for n in range(bands):
                re, im = block[n, 0].astype(F32), block[n, 1].astype(F32)
                dre, dim = grad[32 * n : 32 * n + 16], grad[32 * n + 16 : 32 * n + 32]
                total = total + weights[q, n : n + 1, :] * (re * dim - im * dre)
            y_acc[plane] = total

        for j, i in [(0, 0), (0, 1), (1, 0), (1, 1)]:
            q = 2 * ((yl + j) % 2) + (c + i) % 2
            for s_ in range(2):
                k = 4 * s_ + q
                arrived(outer.at[k], outer_recv.at[k])
                if s_ == 0:
                    sent.append(send(outer.at[k], above.at[q], down_send.at[q], down_recv.at[q], device(ring - 1, s, yl, c)))
                else:
                    sent.append(send(outer.at[k], below.at[q], up_send.at[q], up_recv.at[q], device(ring + 1, s, yl, c)))
            if j + i > 0:
                arrived(weights.at[q], weight_recv.at[q])
            for s_ in range(2):
                k = 4 * s_ + q
                y_current(outer, k, q, 3 * s_)

        for j, i in [(0, 0), (0, 1), (1, 0), (1, 1)]:
            q = 2 * ((yl + j) % 2) + (c + i) % 2
            arrived(above.at[q], down_recv.at[q])
            arrived(below.at[q], up_recv.at[q])
            arrived(inner.at[q], inner_recv.at[q])
            arrived(inner.at[4 + q], inner_recv.at[4 + q])

            def z_step(n, sums):
                w = weights[q, pl.ds(n, 1), :]

                def field(slots, k):
                    return slots[k, n, 0].astype(F32), slots[k, n, 1].astype(F32)

                def term(u, v):
                    return u[0] * v[1] - u[1] * v[0]

                def weighted(u):
                    return w * u[0], w * u[1]

                a0, b1 = field(outer, q), field(outer, 4 + q)
                a1, b0 = field(inner, q), field(inner, 4 + q)
                nxt, prv = field(above, q), field(below, q)
                wa1, wb0, wn = weighted(a1), weighted(b0), weighted(nxt)
                terms = (
                    term(a0, wa1), term(wa1, b0), term(wb0, b1), term(a0, wb0), term(wa1, b1),
                    term(b1, wn), term(b0, wn), term(prv, wa1),
                )
                return tuple(x + t for x, t in zip(sums, terms))

            sums = lax.fori_loop(0, bands, z_step, tuple(pairs[p] for p in range(8)))
            for p in range(8):
                pairs[p] = sums[p]
            y_current(inner, q, q, 1)
            y_current(inner, 4 + q, q, 2)

        a01, a1b0, b01, a0b0, a1b1, b1n0, b0n0, p1a1 = (pairs[p] for p in range(8))
        near, far = 8.0 / 12.0, 1.0 / 12.0
        extra_out[0] = near * b1n0 - far * b0n0
        extra_out[1] = -far * p1a1
        main_out[0, 0, 0] = near * a01 - far * a0b0
        main_out[0, 0, 1] = near * (a1b0 + a01) - far * (a1b1 + p1a1)
        main_out[1, 0, 0] = near * (b01 + a1b0) - far * (b0n0 + a0b0)
        main_out[1, 0, 1] = near * (b1n0 + b01) - far * a1b1
        for p in range(4):
            main_out[p // 2, 1, p % 2] = y_acc[p] * (1.0 / 12.0)
        for e, r in ((0, ring + 1), (1, ring - 1)):
            sent.append(send(extra_out.at[e], extra_in.at[s], extra_send.at[e], extra_recv.at[s], device(r, e, yo, c)))
        for e in range(2):
            sent.append(send(main_out.at[e], main_in.at[s], main_send.at[e], main_recv.at[s], device(ring, e, yo, c)))

        total = x_acc[:, pl.ds(pl.multiple_of(32 * b, 32), 32), :]
        for j in range(1, 4):
            q = (b + j) % 4
            arrived(x_in.at[q], x_recv.at[q])
            total = total + x_in[q]
        out[1] = total * (1.0 / 12.0)
        for h in range(2):
            rows = slice(16 * h, 16 * h + 16)
            arrived(main_in.at[h], main_recv.at[h])
            arrived(extra_in.at[h], extra_recv.at[h])
            out[0, :, rows, :] = main_in[h, 0]
            out[2, :, rows, :] = main_in[h, 1]
            out[0, s, rows, :] += extra_in[h]
        for copy in sent:
            copy.wait_send()

    return kernel


def solution(mesh):
    rings = mesh.shape["grid"] // 2

    def per_device(orbitals, occupations):
        n = orbitals.shape[0]
        dma = pltpu.SemaphoreType.DMA
        chunk = (n, 2, 16, 128)
        return pl.pallas_call(
            make_kernel(rings),
            out_shape=pltpu.VMEM((3, 2, 32, 128), F32),
            in_specs=[pl.BlockSpec(memory_space=pl.ANY), pl.BlockSpec(memory_space=pl.ANY)],
            out_specs=pl.BlockSpec(memory_space=pltpu.VMEM),
            scratch_shapes=[
                pltpu.SMEM((n,), F32),
                pltpu.VMEM((n, 2, 2, 128, 128), BF16),
                pltpu.VMEM((8, *chunk), BF16),
                pltpu.VMEM((8, *chunk), BF16),
                pltpu.VMEM((4, *chunk), BF16),
                pltpu.VMEM((4, *chunk), BF16),
                pltpu.VMEM((4, n, 128), F32),
                pltpu.VMEM((128, 128), BF16),
                pltpu.VMEM((128, 128), BF16),
                pltpu.VMEM((2, 128, 128), F32),
                pltpu.VMEM((4, 2, 32, 128), F32),
                pltpu.VMEM((4, 16, 128), F32),
                pltpu.VMEM((8, 16, 128), F32),
                pltpu.VMEM((2, 2, 2, 16, 128), F32),
                pltpu.VMEM((2, 2, 2, 16, 128), F32),
                pltpu.VMEM((2, 16, 128), F32),
                pltpu.VMEM((2, 16, 128), F32),
                dma,
                dma((2,)),
                dma((7,)), dma((8,)),
                dma((7,)), dma((8,)),
                dma((4,)), dma((4,)),
                dma((4,)), dma((4,)),
                dma((3,)), dma((4,)),
                dma((3,)), dma((4,)),
                dma((2,)), dma((2,)),
                dma((2,)), dma((2,)),
            ],
            compiler_params=pltpu.CompilerParams(collective_id=0, has_side_effects=True),
        )(orbitals, occupations)

    return jax.shard_map(
        per_device,
        mesh=mesh,
        in_specs=(P("band", None, "grid", None, None), P("band")),
        out_specs=P(None, "grid", "band", None),
        check_vma=False,
    )
```

```python
import jax
import jax.numpy as jnp
from jax import lax
from jax.experimental import pallas as pl
from jax.experimental.pallas import tpu as pltpu
from jax.sharding import PartitionSpec as P

MESH = pl.DeviceIdType.MESH
F32 = jnp.float32
BF16 = jnp.bfloat16


def stencil(n, transposed):
    i = lax.broadcasted_iota(jnp.int32, (n, n), 0)
    j = lax.broadcasted_iota(jnp.int32, (n, n), 1)
    d = (i - j if transposed else j - i) + n
    d = jnp.where(d >= n, d - n, d)
    near = jnp.where(d == 1, 8.0, 0.0) - jnp.where(d == n - 1, 8.0, 0.0)
    far = jnp.where(d == n - 2, 1.0, 0.0) - jnp.where(d == 2, 1.0, 0.0)
    return (near + far).astype(BF16)


def make_kernel(rings):
    def kernel(
        orb, occ_in, out,
        occ, own, outer, late, weights, mat_x, mat_y,
        x_acc, x_in, y_acc, pairs, main_out, main_in, extra_out, extra_in,
        occ_sem, load_sem, send_sem, outer_sem, late_sem, weight_sem, x_sem, main_sem, extra_sem, up_ready, down_ready,
    ):
        bands = own.shape[0]
        b = lax.axis_index("band")
        g = lax.axis_index("grid")
        ring, s = g // 2, g % 2
        yl, c = b // 2, b % 2
        yo, co = 1 - yl, 1 - c
        turn = ring % 4

        def device(r, s_, yl_, c_):
            return {"band": 2 * yl_ + c_, "grid": 2 * ((r + rings) % rings) + s_}

        flips = [(0, 0, 1), (1, 0, 0), (1, 0, 1), (0, 1, 0), (1, 1, 0), (0, 1, 1), (1, 1, 1)]
        peers = [((s + i) % 2, (yl + j) % 2, (c + k) % 2) for i, j, k in flips]
        above, below = device(ring + 1, s, yl, c), device(ring - 1, s, yl, c)
        barrier = pltpu.get_barrier_semaphore()

        def signal(sem, target):
            pl.semaphore_signal(sem, inc=1, device_id=target, device_id_type=MESH)

        for s_, yl_, c_ in peers:
            signal(barrier, device(ring, s_, yl_, c_))
        pl.when(turn != 3)(lambda: signal(barrier, above))
        pl.when(turn == 0)(lambda: signal(barrier, below))

        occ_load = pltpu.make_async_copy(occ_in, occ, occ_sem)
        loads = [
            pltpu.make_async_copy(orb.at[:, :, plane], own.at[:, :, plane], load_sem.at[k])
            for k, plane in enumerate((s, 1 - s))
        ]
        loads[0].start()
        occ_load.start()
        loads[1].start()

        def my_rows(s_, yl_, c_):
            return pl.ds(pl.multiple_of(32 * (2 * (1 - yl_) + 1 - c_) + 16 * s_, 16), 16)

        mine = my_rows(s, yl, c)
        pltpu.make_async_copy(orb.at[:, :, s, mine, :], outer.at[b, s], outer_sem.at[b]).start()
        pltpu.make_async_copy(orb.at[:, :, 1 - s, mine, :], late.at[b, s], late_sem.at[b]).start()
        mat_x[...] = stencil(128, False)
        mat_y[...] = stencil(128, True)
        x_acc[...] = jnp.zeros_like(x_acc)
        y_acc[...] = jnp.zeros_like(y_acc)
        pairs[...] = jnp.zeros_like(pairs)
        occ_load.wait()
        for n in range(bands):
            weights[b, n : n + 1, :] = jnp.full((1, 128), occ[n], F32)
        loads[0].wait()
        pl.semaphore_wait(barrier, 7 + (turn + 1) // 2)

        sent = []

        def send(src, dst, sem, target):
            copy = pltpu.make_async_remote_copy(
                src_ref=src, dst_ref=dst, send_sem=send_sem, recv_sem=sem, device_id=target, device_id_type=MESH
            )
            copy.start()
            sent.append(copy)

        def arrived(ref, sem):
            pltpu.make_async_copy(ref, ref, sem).wait()

        for j, i in [(0, 1), (1, 0), (1, 1)]:
            send(weights.at[b], weights.at[b], weight_sem, device(ring, s, (yl + j) % 2, (c + i) % 2))
        for s_, yl_, c_ in peers:
            send(own.at[:, :, s, my_rows(s_, yl_, c_), :], outer.at[b, s], outer_sem.at[b], device(ring, s_, yl_, c_))
        pl.when(turn != 0)(lambda: signal(up_ready, below))
        pl.when(turn == 3)(lambda: signal(down_ready, above))
        loads[1].wait()

        def x_step(n, _):
            w = occ[n]
            for z in range(2):
                re = own[n, 0, z]
                im = own[n, 1, z]
                dre = jnp.dot(mat_x[...], re, preferred_element_type=F32)
                dim = jnp.dot(mat_x[...], im, preferred_element_type=F32)
                x_acc[z] += w * (re.astype(F32) * dim - im.astype(F32) * dre)
            return 0

        lax.fori_loop(0, bands, x_step, 0)

        for s_, yl_, c_ in peers:
            send(own.at[:, :, 1 - s, my_rows(s_, yl_, c_), :], late.at[b, s], late_sem.at[b], device(ring, s_, yl_, c_))
        for j in range(1, 4):
            to = (b + j) % 4
            rows = pl.ds(pl.multiple_of(32 * to, 32), 32)
            send(x_acc.at[:, rows, :], x_in.at[b], x_sem, device(ring, s, to // 2, to % 2))

        arrived(weights.at[pl.ds(0, 3)], weight_sem)
        pl.when(turn != 3)(lambda: pl.semaphore_wait(up_ready, 1))
        pl.when(turn == 0)(lambda: pl.semaphore_wait(down_ready, 1))

        def y_current(slots, q, k, plane):
            block = slots[q, k]
            grad = jnp.dot(block.reshape(bands * 32, 128), mat_y[...], preferred_element_type=F32)
            total = y_acc[plane]
            for n in range(bands):
                re, im = block[n, 0].astype(F32), block[n, 1].astype(F32)
                dre, dim = grad[32 * n : 32 * n + 16], grad[32 * n + 16 : 32 * n + 32]
                total = total + weights[q, n : n + 1, :] * (re * dim - im * dre)
            y_acc[plane] = total

        order = [2 * ((yl + j) % 2) + (c + i) % 2 for j, i in [(0, 0), (0, 1), (1, 0), (1, 1)]]

        for q in order:
            arrived(outer.at[q], outer_sem.at[q])
            send(outer.at[q, 0], late.at[q, 2], late_sem.at[q], below)
            send(outer.at[q, 1], late.at[q, 3], late_sem.at[q], above)
            y_current(outer, q, 0, 0)
            y_current(outer, q, 1, 3)

        def to_owner(e, part, size):
            send(main_out.at[e, pl.ds(part, size)], main_in.at[s, pl.ds(part, size)], main_sem, device(ring, e, yo, co))

        near, far = 8.0 / 12.0, 1.0 / 12.0
        for e in range(2):
            main_out[e, 2] = far * y_acc[3 * e]
            to_owner(e, 2, 1)

        def pair_sums(q, picked):
            def z_step(n, sums):
                w = weights[q, pl.ds(n, 1), :]

                def field(slots, k):
                    return slots[q, k, n, 0].astype(F32), slots[q, k, n, 1].astype(F32)

                def term(u, v):
                    return u[0] * v[1] - u[1] * v[0]

                def weighted(u):
                    return w * u[0], w * u[1]

                a0, b1 = field(outer, 0), field(outer, 1)
                a1, b0, nxt, prv = field(late, 0), field(late, 1), field(late, 2), field(late, 3)
                wa1, wb0, wn = weighted(a1), weighted(b0), weighted(nxt)
                terms = [
                    (b1, wn), (b0, wn), (prv, wa1), (a0, wa1), (wa1, b0), (wb0, b1), (a0, wb0), (wa1, b1),
                ]
                return tuple(x + term(*terms[p]) for x, p in zip(sums, picked))

            sums = lax.fori_loop(0, bands, z_step, tuple(pairs[p] for p in picked), unroll=4)
            for p, x in zip(picked, sums):
                pairs[p] = x

        for q in order[:3]:
            arrived(late.at[q], late_sem.at[q])
            pair_sums(q, range(8))
            y_current(late, q, 0, 1)
            y_current(late, q, 1, 2)
        q = order[3]
        arrived(late.at[q], late_sem.at[q])
        pair_sums(q, range(3))
        b1n0, b0n0, p1a1 = (pairs[p] for p in range(3))
        extra_out[0] = near * b1n0 - far * b0n0
        extra_out[1] = -far * p1a1
        for e, r in ((0, ring + 1), (1, ring - 1)):
            send(extra_out.at[e], extra_in.at[s], extra_sem, device(r, e, yo, co))
        pair_sums(q, range(3, 8))
        a01, a1b0, b01, a0b0, a1b1 = (pairs[p] for p in range(3, 8))
        main_out[0, 0] = near * a01 - far * a0b0
        main_out[0, 1] = near * (a1b0 + a01) - far * (a1b1 + p1a1)
        main_out[1, 0] = near * (b01 + a1b0) - far * (b0n0 + a0b0)
        main_out[1, 1] = near * (b1n0 + b01) - far * a1b1
        for e in range(2):
            to_owner(e, 0, 2)
        y_current(late, q, 0, 1)
        y_current(late, q, 1, 2)
        for e in range(2):
            main_out[e, 3] = far * y_acc[1 + e]
            to_owner(e, 3, 1)

        arrived(x_in.at[pl.ds(0, 3)], x_sem)
        total = x_acc[:, pl.ds(pl.multiple_of(32 * b, 32), 32), :]
        for j in range(1, 4):
            total = total + x_in[(b + j) % 4]
        out[1] = total * far
        arrived(main_in, main_sem)
        arrived(extra_in, extra_sem)
        for h in range(2):
            rows = slice(16 * h, 16 * h + 16)
            out[0, :, rows, :] = main_in[h, :2]
            out[2, s, rows, :] = main_in[h, 2]
            out[2, 1 - s, rows, :] = main_in[h, 3]
            out[0, s, rows, :] += extra_in[h]
        for copy in sent:
            copy.wait_send()

    return kernel


def solution(mesh):
    rings = mesh.shape["grid"] // 2

    def per_device(orbitals, occupations):
        n = orbitals.shape[0]
        dma = pltpu.SemaphoreType.DMA
        chunk = (n, 2, 16, 128)
        return pl.pallas_call(
            make_kernel(rings),
            out_shape=pltpu.VMEM((3, 2, 32, 128), F32),
            in_specs=[pl.BlockSpec(memory_space=pl.ANY), pl.BlockSpec(memory_space=pl.ANY)],
            out_specs=pl.BlockSpec(memory_space=pltpu.VMEM),
            scratch_shapes=[
                pltpu.SMEM((n,), F32),
                pltpu.VMEM((n, 2, 2, 128, 128), BF16),
                pltpu.VMEM((4, 2, *chunk), BF16),
                pltpu.VMEM((4, 4, *chunk), BF16),
                pltpu.VMEM((4, n, 128), F32),
                pltpu.VMEM((128, 128), BF16),
                pltpu.VMEM((128, 128), BF16),
                pltpu.VMEM((2, 128, 128), F32),
                pltpu.VMEM((4, 2, 32, 128), F32),
                pltpu.VMEM((4, 16, 128), F32),
                pltpu.VMEM((8, 16, 128), F32),
                pltpu.VMEM((2, 4, 16, 128), F32),
                pltpu.VMEM((2, 4, 16, 128), F32),
                pltpu.VMEM((2, 16, 128), F32),
                pltpu.VMEM((2, 16, 128), F32),
                dma, dma((2,)), dma, dma((4,)), dma((4,)), dma, dma, dma, dma,
                pltpu.SemaphoreType.REGULAR, pltpu.SemaphoreType.REGULAR,
            ],
            compiler_params=pltpu.CompilerParams(collective_id=0, has_side_effects=True),
        )(orbitals, occupations)

    return jax.shard_map(
        per_device,
        mesh=mesh,
        in_specs=(P("band", None, "grid", None, None), P("band")),
        out_specs=P(None, "grid", "band", None),
        check_vma=False,
    )
```

```python
import jax
import jax.numpy as jnp
from jax import lax
from jax.experimental import pallas as pl
from jax.experimental.pallas import tpu as pltpu
from jax.sharding import PartitionSpec as P

MESH = pl.DeviceIdType.MESH
F32 = jnp.float32
BF16 = jnp.bfloat16


def stencil(n, transposed):
    i = lax.broadcasted_iota(jnp.int32, (n, n), 0)
    j = lax.broadcasted_iota(jnp.int32, (n, n), 1)
    d = (i - j if transposed else j - i) + n
    d = jnp.where(d >= n, d - n, d)
    near = jnp.where(d == 1, 8.0, 0.0) - jnp.where(d == n - 1, 8.0, 0.0)
    far = jnp.where(d == n - 2, 1.0, 0.0) - jnp.where(d == 2, 1.0, 0.0)
    return (near + far).astype(BF16)


INNER = [(0, 0, 1), (1, 0, 0), (1, 0, 1), (0, 1, 0), (1, 1, 0), (0, 1, 1), (1, 1, 1)]


def EARLY(ring, rings):
    return ring == 0, ring == rings - 1


def make_kernel(rings):
    def kernel(
        orb, occ_in, out,
        occ, own, outer, late, weights, mat_x, mat_y,
        x_acc, x_in, y_acc, pairs, main_out, main_in, extra_out, extra_in, tip_in, relay_in, tip_sums,
        occ_sem, load_sem, send_sem, outer_sem, edge_sem, same_sem, cross_sem, weight_sem, x_sem, main_sem, extra_sem, tip_sem, relay_sem, sums_sem,
        up_ready, down_ready,
    ):
        bands = own.shape[0]
        b = lax.axis_index("band")
        g = lax.axis_index("grid")
        ring, s = g // 2, g % 2
        yl, c = b // 2, b % 2
        yo, co = 1 - yl, 1 - c
        turn = ring % 4

        def device(r, s_, yl_, c_):
            return {"band": 2 * yl_ + c_, "grid": 2 * ((r + rings) % rings) + s_}

        flips = [(0, 0, 1), (1, 0, 0), (1, 0, 1), (0, 1, 0), (1, 1, 0), (0, 1, 1), (1, 1, 1)]
        peers = [((s + i) % 2, (yl + j) % 2, (c + k) % 2) for i, j, k in flips]
        above, below = device(ring + 1, s, yl, c), device(ring - 1, s, yl, c)
        barrier = pltpu.get_barrier_semaphore()

        def signal(sem, target):
            pl.semaphore_signal(sem, inc=1, device_id=target, device_id_type=MESH)

        for s_, yl_, c_ in peers:
            signal(barrier, device(ring, s_, yl_, c_))
        pl.when(turn != 3)(lambda: signal(barrier, above))
        pl.when(turn == 0)(lambda: signal(barrier, below))
        early, ahead = EARLY(ring, rings)
        tip_turn, relay_turn = ahead & (s == 1), early & (s == 1)

        occ_load = pltpu.make_async_copy(occ_in, occ, occ_sem)
        loads = [
            pltpu.make_async_copy(orb.at[:, :, plane], own.at[:, :, plane], load_sem.at[k])
            for k, plane in enumerate((s, 1 - s))
        ]
        loads[0].start()
        occ_load.start()
        loads[1].start()

        def my_rows(s_, yl_, c_):
            return pl.ds(pl.multiple_of(32 * (2 * (1 - yl_) + 1 - c_) + 16 * s_, 16), 16)

        mine = my_rows(s, yl, c)
        pltpu.make_async_copy(orb.at[:, :, s, mine, :], outer.at[b, s], outer_sem.at[b]).start()
        pltpu.make_async_copy(orb.at[:, :, 1 - s, mine, :], late.at[b, s], same_sem.at[b]).start()
        mat_x[...] = stencil(128, False)
        mat_y[...] = stencil(128, True)
        x_acc[...] = jnp.zeros_like(x_acc)
        y_acc[...] = jnp.zeros_like(y_acc)
        pairs[...] = jnp.zeros_like(pairs)
        occ_load.wait()
        for n in range(bands):
            weights[b, n : n + 1, :] = jnp.full((1, 128), occ[n], F32)
        loads[0].wait()
        pl.semaphore_wait(barrier, 7 + (turn + 1) // 2)

        def start(src, dst, sem, target):
            copy = pltpu.make_async_remote_copy(
                src_ref=src, dst_ref=dst, send_sem=send_sem, recv_sem=sem, device_id=target, device_id_type=MESH
            )
            copy.start()
            return copy

        sent = []

        def send(*args):
            sent.append(start(*args))

        def arrived(ref, sem):
            pltpu.make_async_copy(ref, ref, sem).wait()

        for j, i in [(0, 1), (1, 0), (1, 1)]:
            send(weights.at[b], weights.at[b], weight_sem, device(ring, s, (yl + j) % 2, (c + i) % 2))
        def tip_copy(e):
            return (own.at[:, :, 0, my_rows(e, yo, co), :], relay_in.at[e], relay_sem, above)

        def sums_copy():
            return (extra_out.at[2], tip_sums.at[s], sums_sem, device(ring, 0, yo, co))

        def relay_copy(e):
            return (relay_in.at[e], tip_in, tip_sem, device(ring, e, yo, co))

        @pl.when(tip_turn)
        def _():
            loads[1].wait()
            for e in range(2):
                start(*tip_copy(e))

        for s_, yl_, c_ in peers:
            send(own.at[:, :, s, my_rows(s_, yl_, c_), :], outer.at[b, s], outer_sem.at[b], device(ring, s_, yl_, c_))
        pl.when(turn != 0)(lambda: signal(up_ready, below))
        pl.when(turn == 3)(lambda: signal(down_ready, above))
        pl.when(jnp.logical_not(tip_turn))(lambda: loads[1].wait())

        def x_step(n, _):
            w = occ[n]
            for z in range(2):
                re = own[n, 0, z]
                im = own[n, 1, z]
                dre = jnp.dot(mat_x[...], re, preferred_element_type=F32)
                dim = jnp.dot(mat_x[...], im, preferred_element_type=F32)
                x_acc[z] += w * (re.astype(F32) * dim - im.astype(F32) * dre)
            return 0

        lax.fori_loop(0, bands, x_step, 0)

        pl.when(turn != 3)(lambda: pl.semaphore_wait(up_ready, 1))
        pl.when(turn == 0)(lambda: pl.semaphore_wait(down_ready, 1))
        for i, j, k in INNER:
            s_, yl_, c_ = (s + i) % 2, (yl + j) % 2, (c + k) % 2
            sem = (cross_sem if i else same_sem).at[b]
            send(own.at[:, :, 1 - s, my_rows(s_, yl_, c_), :], late.at[b, s], sem, device(ring, s_, yl_, c_))
        for j in range(1, 4):
            to = (b + j) % 4
            rows = pl.ds(pl.multiple_of(32 * to, 32), 32)
            send(x_acc.at[:, rows, :], x_in.at[b], x_sem, device(ring, s, to // 2, to % 2))

        arrived(weights.at[pl.ds(0, 3)], weight_sem)

        def y_current(slots, q, k, plane):
            block = slots[q, k]
            grad = jnp.dot(block.reshape(bands * 32, 128), mat_y[...], preferred_element_type=F32)
            total = y_acc[plane]
            for n in range(bands):
                re, im = block[n, 0].astype(F32), block[n, 1].astype(F32)
                dre, dim = grad[32 * n : 32 * n + 16], grad[32 * n + 16 : 32 * n + 32]
                total = total + weights[q, n : n + 1, :] * (re * dim - im * dre)
            y_acc[plane] = total

        order = [2 * ((yl + j) % 2) + (c + i) % 2 for j, i in [(0, 0), (0, 1), (1, 0), (1, 1)]]

        for q in order:
            arrived(outer.at[q], outer_sem.at[q])
            send(outer.at[q, 0], late.at[q, 2], edge_sem.at[q], below)
            send(outer.at[q, 1], late.at[q, 3], edge_sem.at[q], above)
            y_current(outer, q, 0, 0)
            y_current(outer, q, 1, 3)

        def to_owner(e, part, size):
            send(main_out.at[e, pl.ds(part, size)], main_in.at[s, pl.ds(part, size)], main_sem, device(ring, e, yo, co))

        near, far = 8.0 / 12.0, 1.0 / 12.0
        for e in range(2):
            main_out[e, 2] = far * y_acc[3 * e]
            to_owner(e, 2, 1)

        def term(u, v):
            return u[0] * v[1] - u[1] * v[0]

        names = [
            ("b1", "nxt"), ("b0", "nxt"), ("a1", "prv"), ("a1", "a0"), ("a1", "b0"), ("b0", "b1"), ("b0", "a0"), ("a1", "b1"),
        ]
        places = {"a0": (outer, 0), "b1": (outer, 1), "a1": (late, 0), "b0": (late, 1), "nxt": (late, 2), "prv": (late, 3)}

        def pair_sums(q, picked):
            def z_step(n, sums):
                w = weights[q, pl.ds(n, 1), :]
                used = sorted({name for p in picked for name in names[p]})
                field = {}
                for name in used:
                    slots, k = places[name]
                    field[name] = (slots[q, k, n, 0].astype(F32), slots[q, k, n, 1].astype(F32))
                scaled = {name: (w * field[name][0], w * field[name][1]) for name in sorted({names[p][0] for p in picked})}
                return tuple(x + term(scaled[names[p][0]], field[names[p][1]]) for x, p in zip(sums, picked))

            sums = lax.fori_loop(0, bands, z_step, tuple(pairs[p] for p in picked), unroll=4)
            for p, x in zip(picked, sums):
                pairs[p] = x

        @pl.when(relay_turn)
        def _():
            arrived(relay_in, relay_sem)
            for e in range(2):
                start(*relay_copy(e))

        def edge_up():
            extra_out[0] = near * pairs[0] - far * pairs[1]
            start(extra_out.at[0], extra_in.at[s], extra_sem, device(ring + 1, 0, yo, co))

        def now(q, *picked):
            pair_sums(q, picked)
            edge_up()

        for q in order[:3]:
            arrived(late.at[q, pl.ds(2, 2)], edge_sem.at[q])
            arrived(late.at[q, 0], same_sem.at[q])
            arrived(late.at[q, 1], cross_sem.at[q])
            pair_sums(q, range(8))
            y_current(late, q, 0, 1)
            y_current(late, q, 1, 2)
        q = order[3]
        arrived(late.at[q, pl.ds(2, 2)], edge_sem.at[q])
        pl.when(ahead)(lambda: now(q, 0))
        arrived(late.at[q, 0], same_sem.at[q])
        arrived(late.at[q, 1], cross_sem.at[q])
        pl.when(ahead)(lambda: pair_sums(q, (1,)))
        pl.when(jnp.logical_not(ahead))(lambda: now(q, 0, 1))
        pair_sums(q, (2,))
        b1n0, b0n0, p1a1 = pairs[0], pairs[1], -pairs[2]
        extra_out[1] = -far * p1a1
        send(extra_out.at[1], extra_in.at[s], extra_sem, device(ring - 1, 1, yo, co))
        pair_sums(q, range(3, 8))
        a01, a1b0, b01, a0b0, a1b1 = -pairs[3], pairs[4], pairs[5], -pairs[6], pairs[7]
        main_out[0, 0] = near * a01 - far * a0b0
        main_out[0, 1] = near * (a1b0 + a01) - far * (a1b1 + p1a1)
        main_out[1, 0] = near * (b01 + a1b0) - far * (b0n0 + a0b0)
        main_out[1, 1] = near * (b1n0 + b01) - far * a1b1
        for e in range(2):
            to_owner(e, 0, 2)
        y_current(late, q, 0, 1)
        y_current(late, q, 1, 2)
        for e in range(2):
            main_out[e, 3] = far * y_acc[1 + e]
            to_owner(e, 3, 1)

        @pl.when(early)
        def _():
            arrived(tip_in, tip_sem)

            def step(n, total):
                w = weights[q, pl.ds(n, 1), :]
                here = [w * outer[q, 0, n, p].astype(F32) for p in range(2)]
                there = [tip_in[n, p].astype(F32) for p in range(2)]
                return total + term(there, here)

            extra_out[2] = -far * lax.fori_loop(0, bands, step, jnp.zeros((16, 128), F32), unroll=4)
            start(*sums_copy())

        arrived(x_in.at[pl.ds(0, 3)], x_sem)
        total = x_acc[:, pl.ds(pl.multiple_of(32 * b, 32), 32), :]
        for j in range(1, 4):
            total = total + x_in[(b + j) % 4]
        out[1] = total * far
        arrived(main_in, main_sem)
        arrived(extra_in, extra_sem)
        for h in range(2):
            rows = slice(16 * h, 16 * h + 16)
            out[0, :, rows, :] = main_in[h, :2]
            out[2, s, rows, :] = main_in[h, 2]
            out[2, 1 - s, rows, :] = main_in[h, 3]
            out[0, s, rows, :] += extra_in[h]

        @pl.when(early & (s == 0))
        def _():
            arrived(tip_sums, sums_sem)
            for h in range(2):
                out[0, 0, 16 * h : 16 * h + 16, :] += tip_sums[h]

        def sent_copy(src, dst, sem, target):
            pltpu.make_async_remote_copy(
                src_ref=src, dst_ref=dst, send_sem=send_sem, recv_sem=sem, device_id=target, device_id_type=MESH
            ).wait_send()

        sent_copy(extra_out.at[0], extra_in.at[s], extra_sem, device(ring + 1, 0, yo, co))

        pl.when(early)(lambda: sent_copy(*sums_copy()))
        for turn_, copies in ((tip_turn, tip_copy), (relay_turn, relay_copy)):

            @pl.when(turn_)
            def _():
                for e in range(2):
                    sent_copy(*copies(e))

        for copy in sent:
            copy.wait_send()

    return kernel


def solution(mesh):
    rings = mesh.shape["grid"] // 2

    def per_device(orbitals, occupations):
        n = orbitals.shape[0]
        dma = pltpu.SemaphoreType.DMA
        chunk = (n, 2, 16, 128)
        return pl.pallas_call(
            make_kernel(rings),
            out_shape=pltpu.VMEM((3, 2, 32, 128), F32),
            in_specs=[pl.BlockSpec(memory_space=pl.ANY), pl.BlockSpec(memory_space=pl.ANY)],
            out_specs=pl.BlockSpec(memory_space=pltpu.VMEM),
            scratch_shapes=[
                pltpu.SMEM((n,), F32),
                pltpu.VMEM((n, 2, 2, 128, 128), BF16),
                pltpu.VMEM((4, 2, *chunk), BF16),
                pltpu.VMEM((4, 4, *chunk), BF16),
                pltpu.VMEM((4, n, 128), F32),
                pltpu.VMEM((128, 128), BF16),
                pltpu.VMEM((128, 128), BF16),
                pltpu.VMEM((2, 128, 128), F32),
                pltpu.VMEM((4, 2, 32, 128), F32),
                pltpu.VMEM((4, 16, 128), F32),
                pltpu.VMEM((8, 16, 128), F32),
                pltpu.VMEM((2, 4, 16, 128), F32),
                pltpu.VMEM((2, 4, 16, 128), F32),
                pltpu.VMEM((3, 16, 128), F32),
                pltpu.VMEM((2, 16, 128), F32),
                pltpu.VMEM(chunk, BF16),
                pltpu.VMEM((2, *chunk), BF16),
                pltpu.VMEM((2, 16, 128), F32),
                dma, dma((2,)), dma, dma((4,)), dma((4,)), dma((4,)), dma((4,)), dma, dma, dma, dma, dma, dma, dma,
                pltpu.SemaphoreType.REGULAR, pltpu.SemaphoreType.REGULAR,
            ],
            compiler_params=pltpu.CompilerParams(collective_id=0, has_side_effects=True),
        )(orbitals, occupations)

    return jax.shard_map(
        per_device,
        mesh=mesh,
        in_specs=(P("band", None, "grid", None, None), P("band")),
        out_specs=P(None, "grid", "band", None),
        check_vma=False,
    )
```

```python
import jax
import jax.numpy as jnp
from jax import lax
from jax.experimental import pallas as pl
from jax.experimental.pallas import tpu as pltpu
from jax.sharding import PartitionSpec as P

MESH = pl.DeviceIdType.MESH
F32 = jnp.float32
BF16 = jnp.bfloat16


def stencil(n, transposed):
    i = lax.broadcasted_iota(jnp.int32, (n, n), 0)
    j = lax.broadcasted_iota(jnp.int32, (n, n), 1)
    d = (i - j if transposed else j - i) + n
    d = jnp.where(d >= n, d - n, d)
    near = jnp.where(d == 1, 8.0, 0.0) - jnp.where(d == n - 1, 8.0, 0.0)
    far = jnp.where(d == n - 2, 1.0, 0.0) - jnp.where(d == 2, 1.0, 0.0)
    return (near + far).astype(BF16)


OUTER = [(0, 0, 1), (1, 0, 0), (1, 0, 1), (0, 1, 0), (1, 1, 0), (0, 1, 1), (1, 1, 1)]
INNER = [(0, 0, 1), (0, 1, 0), (1, 1, 0), (0, 1, 1), (1, 1, 1), (1, 0, 0), (1, 0, 1)]
OUTER_USE = [(0, 0), (0, 1), (1, 0), (1, 1)]
INNER_USE = [(1, 0), (1, 1), (0, 0), (0, 1)]
SAME_USE = [(0, 0), (0, 1), (1, 0), (1, 1)]


def EARLY(ring, rings):
    return ring == 0, ring == rings - 1


def make_kernel(rings):
    def kernel(
        orb, occ_in, out,
        occ, own, outer, late, weights, mat_x, mat_y,
        x_acc, x_in, y_acc, pairs, main_out, main_in, extra_out, extra_in, tip_in, relay_in, tip_sums,
        occ_sem, load_sem, send_sem, outer_sem, edge_sem, same_sem, cross_sem, weight_sem, x_sem, main_sem, extra_sem, tip_sem, relay_sem, sums_sem,
        up_ready, down_ready,
    ):
        bands = own.shape[0]
        b = lax.axis_index("band")
        g = lax.axis_index("grid")
        ring, s = g // 2, g % 2
        yl, c = b // 2, b % 2
        yo, co = 1 - yl, 1 - c
        turn = ring % 4

        def device(r, s_, yl_, c_):
            return {"band": 2 * yl_ + c_, "grid": 2 * ((r + rings) % rings) + s_}

        peers = [((s + i) % 2, (yl + j) % 2, (c + k) % 2) for i, j, k in OUTER]
        above, below = device(ring + 1, s, yl, c), device(ring - 1, s, yl, c)
        barrier = pltpu.get_barrier_semaphore()

        def signal(sem, target):
            pl.semaphore_signal(sem, inc=1, device_id=target, device_id_type=MESH)

        for s_, yl_, c_ in peers:
            signal(barrier, device(ring, s_, yl_, c_))
        pl.when(turn != 3)(lambda: signal(barrier, above))
        pl.when(turn == 0)(lambda: signal(barrier, below))
        early, ahead = EARLY(ring, rings)
        tip_turn, relay_turn = ahead & (s == 1), early & (s == 1)

        occ_load = pltpu.make_async_copy(occ_in, occ, occ_sem)
        loads = [
            pltpu.make_async_copy(orb.at[:, :, plane], own.at[:, :, plane], load_sem.at[k])
            for k, plane in enumerate((s, 1 - s))
        ]
        loads[0].start()
        occ_load.start()
        loads[1].start()

        def my_rows(s_, yl_, c_):
            return pl.ds(pl.multiple_of(32 * (2 * (1 - yl_) + 1 - c_) + 16 * s_, 16), 16)

        mine = my_rows(s, yl, c)
        pltpu.make_async_copy(orb.at[:, :, s, mine, :], outer.at[b, s], outer_sem.at[b]).start()
        pltpu.make_async_copy(orb.at[:, :, 1 - s, mine, :], late.at[b, s], same_sem.at[b]).start()
        mat_x[...] = stencil(128, False)
        mat_y[...] = stencil(128, True)
        x_acc[...] = jnp.zeros_like(x_acc)
        y_acc[...] = jnp.zeros_like(y_acc)
        pairs[...] = jnp.zeros_like(pairs)
        occ_load.wait()
        for n in range(bands):
            weights[b, n : n + 1, :] = jnp.full((1, 128), occ[n], F32)
        loads[0].wait()
        pl.semaphore_wait(barrier, 7 + (turn + 1) // 2)

        def start(src, dst, sem, target):
            copy = pltpu.make_async_remote_copy(
                src_ref=src, dst_ref=dst, send_sem=send_sem, recv_sem=sem, device_id=target, device_id_type=MESH
            )
            copy.start()
            return copy

        sent = []

        def send(*args):
            sent.append(start(*args))

        def arrived(ref, sem):
            pltpu.make_async_copy(ref, ref, sem).wait()

        for j, i in [(0, 1), (1, 0), (1, 1)]:
            send(weights.at[b], weights.at[b], weight_sem, device(ring, s, (yl + j) % 2, (c + i) % 2))
        late_j, late_i = INNER_USE[3]
        yt, ct = (yl + late_j) % 2, (c + late_i) % 2

        def tip_copy():
            return (own.at[:, :, 0, my_rows(0, yt, ct), :], relay_in, relay_sem, above)

        def sums_copy():
            return (extra_out.at[2], tip_sums, sums_sem, device(ring, 0, yo, co))

        def relay_copy():
            return (relay_in, tip_in, tip_sem, device(ring, 0, yt, ct))

        @pl.when(tip_turn)
        def _():
            loads[1].wait()
            start(*tip_copy())

        for s_, yl_, c_ in peers:
            send(own.at[:, :, s, my_rows(s_, yl_, c_), :], outer.at[b, s], outer_sem.at[b], device(ring, s_, yl_, c_))
        pl.when(turn != 0)(lambda: signal(up_ready, below))
        pl.when(turn == 3)(lambda: signal(down_ready, above))
        pl.when(jnp.logical_not(tip_turn))(lambda: loads[1].wait())

        def x_step(n, _):
            w = occ[n]
            for z in range(2):
                re = own[n, 0, z]
                im = own[n, 1, z]
                dre = jnp.dot(mat_x[...], re, preferred_element_type=F32)
                dim = jnp.dot(mat_x[...], im, preferred_element_type=F32)
                x_acc[z] += w * (re.astype(F32) * dim - im.astype(F32) * dre)
            return 0

        lax.fori_loop(0, bands, x_step, 0)

        pl.when(turn != 3)(lambda: pl.semaphore_wait(up_ready, 1))
        pl.when(turn == 0)(lambda: pl.semaphore_wait(down_ready, 1))
        for i, j, k in INNER:
            s_, yl_, c_ = (s + i) % 2, (yl + j) % 2, (c + k) % 2
            sem = (cross_sem if i else same_sem).at[b]
            send(own.at[:, :, 1 - s, my_rows(s_, yl_, c_), :], late.at[b, s], sem, device(ring, s_, yl_, c_))
        for j in range(1, 4):
            to = (b + j) % 4
            rows = pl.ds(pl.multiple_of(32 * to, 32), 32)
            send(x_acc.at[:, rows, :], x_in.at[b], x_sem, device(ring, s, to // 2, to % 2))

        arrived(weights.at[pl.ds(0, 3)], weight_sem)

        def y_current(slots, q, k, plane):
            block = slots[q, k]
            grad = jnp.dot(block.reshape(bands * 32, 128), mat_y[...], preferred_element_type=F32)
            total = y_acc[plane]
            for n in range(bands):
                re, im = block[n, 0].astype(F32), block[n, 1].astype(F32)
                dre, dim = grad[32 * n : 32 * n + 16], grad[32 * n + 16 : 32 * n + 32]
                total = total + weights[q, n : n + 1, :] * (re * dim - im * dre)
            y_acc[plane] = total

        def groups(flips):
            return [2 * ((yl + j) % 2) + (c + i) % 2 for j, i in flips]

        order = groups(INNER_USE)

        for q in groups(OUTER_USE):
            arrived(outer.at[q], outer_sem.at[q])
            send(outer.at[q, 0], late.at[q, 2], edge_sem.at[q], below)
            send(outer.at[q, 1], late.at[q, 3], edge_sem.at[q], above)
            y_current(outer, q, 0, 0)
            y_current(outer, q, 1, 3)

        def to_owner(e, part, size):
            send(main_out.at[e, pl.ds(part, size)], main_in.at[s, pl.ds(part, size)], main_sem, device(ring, e, yo, co))

        near, far = 8.0 / 12.0, 1.0 / 12.0
        for e in range(2):
            main_out[e, 2] = far * y_acc[3 * e]
            to_owner(e, 2, 1)

        def term(u, v):
            return u[0] * v[1] - u[1] * v[0]

        names = [
            ("b1", "nxt"), ("b0", "nxt"), ("a1", "prv"), ("a1", "a0"), ("a1", "b0"), ("b0", "b1"), ("b0", "a0"), ("a1", "b1"),
        ]
        places = {"a0": (outer, 0), "b1": (outer, 1), "a1": (late, 0), "b0": (late, 1), "nxt": (late, 2), "prv": (late, 3)}

        def pair_sums(q, picked):
            def z_step(n, sums):
                w = weights[q, pl.ds(n, 1), :]
                used = sorted({name for p in picked for name in names[p]})
                field = {}
                for name in used:
                    slots, k = places[name]
                    field[name] = (slots[q, k, n, 0].astype(F32), slots[q, k, n, 1].astype(F32))
                scaled = {name: (w * field[name][0], w * field[name][1]) for name in sorted({names[p][0] for p in picked})}
                return tuple(x + term(scaled[names[p][0]], field[names[p][1]]) for x, p in zip(sums, picked))

            sums = lax.fori_loop(0, bands, z_step, tuple(pairs[p] for p in picked), unroll=4)
            for p, x in zip(picked, sums):
                pairs[p] = x

        @pl.when(relay_turn)
        def _():
            arrived(relay_in, relay_sem)
            start(*relay_copy())

        def edge_up():
            extra_out[0] = near * pairs[0] - far * pairs[1]
            start(extra_out.at[0], extra_in.at[s], extra_sem, device(ring + 1, 0, yo, co))

        def edge_down():
            extra_out[1] = far * pairs[2]
            start(extra_out.at[1], extra_in.at[s], extra_sem, device(ring - 1, 1, yo, co))

        def inner_y(e):
            main_out[e, 3] = far * y_acc[1 + e]
            to_owner(e, 3, 1)

        for q in groups(SAME_USE):
            arrived(late.at[q, pl.ds(2, 2)], edge_sem.at[q])
            arrived(late.at[q, 0], same_sem.at[q])
            pl.when(s == 0)(lambda: pair_sums(q, (2,)))
            pl.when(s == 1)(lambda: pair_sums(q, (0, 1)))
            y_current(late, q, s, 1 + s)
        pl.when(s == 0)(edge_down)
        pl.when(s == 1)(edge_up)
        inner_y(s)

        for k, q in enumerate(order):
            arrived(late.at[q, 0], cross_sem.at[q])

            @pl.when(s == 1)
            def _():
                pair_sums(q, (2,))
                if k == 3:
                    edge_down()

            @pl.when((s == 0) & jnp.logical_not(ahead))
            def _():
                pair_sums(q, (0, 1))
                if k == 3:
                    edge_up()

            @pl.when((s == 0) & ahead)
            def _():
                pair_sums(q, (0, 1) if k < 3 else (1,))
                if k == 2:
                    pair_sums(order[3], (0,))
                    edge_up()

            pair_sums(q, range(3, 8))
            if k < 3:
                y_current(late, q, 1 - s, 2 - s)

        b1n0, b0n0, p1a1 = pairs[0], pairs[1], -pairs[2]
        a01, a1b0, b01, a0b0, a1b1 = -pairs[3], pairs[4], pairs[5], -pairs[6], pairs[7]
        main_out[0, 0] = near * a01 - far * a0b0
        main_out[0, 1] = near * (a1b0 + a01) - far * (a1b1 + p1a1)
        main_out[1, 0] = near * (b01 + a1b0) - far * (b0n0 + a0b0)
        main_out[1, 1] = near * (b1n0 + b01) - far * a1b1
        for e in range(2):
            to_owner(e, 0, 2)
        y_current(late, order[3], 1 - s, 2 - s)
        inner_y(1 - s)

        @pl.when(early & (s == 0))
        def _():
            q = order[3]
            arrived(tip_in, tip_sem)

            def step(n, total):
                w = weights[q, pl.ds(n, 1), :]
                here = [w * outer[q, 0, n, p].astype(F32) for p in range(2)]
                there = [tip_in[n, p].astype(F32) for p in range(2)]
                return total + term(there, here)

            extra_out[2] = -far * lax.fori_loop(0, bands, step, jnp.zeros((16, 128), F32), unroll=4)
            start(*sums_copy())

        arrived(x_in.at[pl.ds(0, 3)], x_sem)
        total = x_acc[:, pl.ds(pl.multiple_of(32 * b, 32), 32), :]
        for j in range(1, 4):
            total = total + x_in[(b + j) % 4]
        out[1] = total * far
        arrived(main_in, main_sem)
        arrived(extra_in, extra_sem)
        for h in range(2):
            rows = slice(16 * h, 16 * h + 16)
            out[0, :, rows, :] = main_in[h, :2]
            out[2, s, rows, :] = main_in[h, 2]
            out[2, 1 - s, rows, :] = main_in[h, 3]
            out[0, s, rows, :] += extra_in[h]

        @pl.when(early & (s == 0))
        def _():
            arrived(tip_sums, sums_sem)
            out[0, 0, :16, :] += tip_sums[...]

        def sent_copy(src, dst, sem, target):
            pltpu.make_async_remote_copy(
                src_ref=src, dst_ref=dst, send_sem=send_sem, recv_sem=sem, device_id=target, device_id_type=MESH
            ).wait_send()

        sent_copy(extra_out.at[0], extra_in.at[s], extra_sem, device(ring + 1, 0, yo, co))
        sent_copy(extra_out.at[1], extra_in.at[s], extra_sem, device(ring - 1, 1, yo, co))
        pl.when(early & (s == 0))(lambda: sent_copy(*sums_copy()))
        pl.when(tip_turn)(lambda: sent_copy(*tip_copy()))
        pl.when(relay_turn)(lambda: sent_copy(*relay_copy()))
        for copy in sent:
            copy.wait_send()

    return kernel


def solution(mesh):
    rings = mesh.shape["grid"] // 2

    def per_device(orbitals, occupations):
        n = orbitals.shape[0]
        dma = pltpu.SemaphoreType.DMA
        chunk = (n, 2, 16, 128)
        return pl.pallas_call(
            make_kernel(rings),
            out_shape=pltpu.VMEM((3, 2, 32, 128), F32),
            in_specs=[pl.BlockSpec(memory_space=pl.ANY), pl.BlockSpec(memory_space=pl.ANY)],
            out_specs=pl.BlockSpec(memory_space=pltpu.VMEM),
            scratch_shapes=[
                pltpu.SMEM((n,), F32),
                pltpu.VMEM((n, 2, 2, 128, 128), BF16),
                pltpu.VMEM((4, 2, *chunk), BF16),
                pltpu.VMEM((4, 4, *chunk), BF16),
                pltpu.VMEM((4, n, 128), F32),
                pltpu.VMEM((128, 128), BF16),
                pltpu.VMEM((128, 128), BF16),
                pltpu.VMEM((2, 128, 128), F32),
                pltpu.VMEM((4, 2, 32, 128), F32),
                pltpu.VMEM((4, 16, 128), F32),
                pltpu.VMEM((8, 16, 128), F32),
                pltpu.VMEM((2, 4, 16, 128), F32),
                pltpu.VMEM((2, 4, 16, 128), F32),
                pltpu.VMEM((3, 16, 128), F32),
                pltpu.VMEM((2, 16, 128), F32),
                pltpu.VMEM(chunk, BF16),
                pltpu.VMEM(chunk, BF16),
                pltpu.VMEM((16, 128), F32),
                dma, dma((2,)), dma, dma((4,)), dma((4,)), dma((4,)), dma((4,)), dma, dma, dma, dma, dma, dma, dma,
                pltpu.SemaphoreType.REGULAR, pltpu.SemaphoreType.REGULAR,
            ],
            compiler_params=pltpu.CompilerParams(collective_id=0, has_side_effects=True),
        )(orbitals, occupations)

    return jax.shard_map(
        per_device,
        mesh=mesh,
        in_specs=(P("band", None, "grid", None, None), P("band")),
        out_specs=P(None, "grid", "band", None),
        check_vma=False,
    )
```

```python
import jax
import jax.numpy as jnp
from jax import lax
from jax.experimental import pallas as pl
from jax.experimental.pallas import tpu as pltpu
from jax.sharding import PartitionSpec as P

MESH = pl.DeviceIdType.MESH
F32 = jnp.float32
BF16 = jnp.bfloat16


def stencil(n, transposed):
    i = lax.broadcasted_iota(jnp.int32, (n, n), 0)
    j = lax.broadcasted_iota(jnp.int32, (n, n), 1)
    d = (i - j if transposed else j - i) + n
    d = jnp.where(d >= n, d - n, d)
    near = jnp.where(d == 1, 8.0, 0.0) - jnp.where(d == n - 1, 8.0, 0.0)
    far = jnp.where(d == n - 2, 1.0, 0.0) - jnp.where(d == 2, 1.0, 0.0)
    return (near + far).astype(BF16)


OUTER = [(0, 0, 1), (1, 0, 0), (1, 0, 1), (0, 1, 0), (1, 1, 0), (0, 1, 1), (1, 1, 1)]
INNER = [(0, 0, 1), (0, 1, 0), (1, 1, 0), (0, 1, 1), (1, 1, 1), (1, 0, 0), (1, 0, 1)]
OUTER_USE = [(0, 0), (0, 1), (1, 0), (1, 1)]
INNER_USE = [(1, 0), (1, 1), (0, 0), (0, 1)]
SAME_USE = [(0, 0), (0, 1), (1, 0), (1, 1)]


def EARLY(ring, rings):
    return ring == 0, ring == rings - 1


def make_kernel(rings):
    def kernel(
        orb, occ_in, out,
        occ, own, outer, late, weights, mat_x, mat_y,
        x_acc, x_in, y_acc, pairs, main_out, main_in, extra_out, extra_in, tip_in, relay_in, tip_sums,
        occ_sem, load_sem, send_sem, outer_sem, edge_sem, same_sem, cross_sem, weight_sem, x_sem, main_sem, extra_sem, tip_sem, relay_sem, sums_sem,
        up_ready, down_ready,
    ):
        bands = own.shape[0]
        b = lax.axis_index("band")
        g = lax.axis_index("grid")
        ring, s = g // 2, g % 2
        yl, c = b // 2, b % 2
        yo, co = 1 - yl, c
        turn = ring % 4

        def device(r, s_, yl_, c_):
            return {"band": 2 * yl_ + c_, "grid": 2 * ((r + rings) % rings) + s_}

        peers = [((s + i) % 2, (yl + j) % 2, (c + k) % 2) for i, j, k in OUTER]
        above, below = device(ring + 1, s, yl, c), device(ring - 1, s, yl, c)
        barrier = pltpu.get_barrier_semaphore()

        def signal(sem, target):
            pl.semaphore_signal(sem, inc=1, device_id=target, device_id_type=MESH)

        for s_, yl_, c_ in peers:
            signal(barrier, device(ring, s_, yl_, c_))
        pl.when(turn != 3)(lambda: signal(barrier, above))
        pl.when(turn == 0)(lambda: signal(barrier, below))
        early, ahead = EARLY(ring, rings)
        tip_turn, relay_turn = ahead & (s == 1), early & (s == 1)

        occ_load = pltpu.make_async_copy(occ_in, occ, occ_sem)
        loads = [
            pltpu.make_async_copy(orb.at[:, :, plane], own.at[:, :, plane], load_sem.at[k])
            for k, plane in enumerate((s, 1 - s))
        ]
        loads[0].start()
        occ_load.start()
        loads[1].start()

        def my_rows(s_, yl_, c_):
            return pl.ds(pl.multiple_of(32 * (2 * (1 - yl_) + c_) + 16 * s_, 16), 16)

        mine = my_rows(s, yl, c)
        pltpu.make_async_copy(orb.at[:, :, s, mine, :], outer.at[b, s], outer_sem.at[b]).start()
        pltpu.make_async_copy(orb.at[:, :, 1 - s, mine, :], late.at[b, s], same_sem.at[b]).start()
        mat_x[...] = stencil(128, False)
        mat_y[...] = stencil(128, True)
        x_acc[...] = jnp.zeros_like(x_acc)
        y_acc[...] = jnp.zeros_like(y_acc)
        pairs[...] = jnp.zeros_like(pairs)
        occ_load.wait()
        for n in range(bands):
            weights[b, n : n + 1, :] = jnp.full((1, 128), occ[n], F32)
        loads[0].wait()
        pl.semaphore_wait(barrier, 7 + (turn + 1) // 2)

        def start(src, dst, sem, target):
            copy = pltpu.make_async_remote_copy(
                src_ref=src, dst_ref=dst, send_sem=send_sem, recv_sem=sem, device_id=target, device_id_type=MESH
            )
            copy.start()
            return copy

        sent = []

        def send(*args):
            sent.append(start(*args))

        def arrived(ref, sem):
            pltpu.make_async_copy(ref, ref, sem).wait()

        for j, i in [(0, 1), (1, 0), (1, 1)]:
            send(weights.at[b], weights.at[b], weight_sem, device(ring, s, (yl + j) % 2, (c + i) % 2))
        late_j, late_i = INNER_USE[3]
        yt, ct = (yl + late_j) % 2, (c + late_i) % 2

        def tip_copy():
            return (own.at[:, :, 0, my_rows(0, yt, ct), :], relay_in, relay_sem, above)

        def sums_copy():
            return (extra_out.at[2], tip_sums, sums_sem, device(ring, 0, yo, co))

        def relay_copy():
            return (relay_in, tip_in, tip_sem, device(ring, 0, yt, ct))

        @pl.when(tip_turn)
        def _():
            loads[1].wait()
            start(*tip_copy())

        for s_, yl_, c_ in peers:
            send(own.at[:, :, s, my_rows(s_, yl_, c_), :], outer.at[b, s], outer_sem.at[b], device(ring, s_, yl_, c_))
        pl.when(turn != 0)(lambda: signal(up_ready, below))
        pl.when(turn == 3)(lambda: signal(down_ready, above))
        pl.when(jnp.logical_not(tip_turn))(lambda: loads[1].wait())

        def x_step(n, _):
            w = occ[n]
            for z in range(2):
                re = own[n, 0, z]
                im = own[n, 1, z]
                dre = jnp.dot(mat_x[...], re, preferred_element_type=F32)
                dim = jnp.dot(mat_x[...], im, preferred_element_type=F32)
                x_acc[z] += w * (re.astype(F32) * dim - im.astype(F32) * dre)
            return 0

        lax.fori_loop(0, bands, x_step, 0)

        pl.when(turn != 3)(lambda: pl.semaphore_wait(up_ready, 1))
        pl.when(turn == 0)(lambda: pl.semaphore_wait(down_ready, 1))
        for i, j, k in INNER:
            s_, yl_, c_ = (s + i) % 2, (yl + j) % 2, (c + k) % 2
            sem = (cross_sem if i else same_sem).at[b]
            send(own.at[:, :, 1 - s, my_rows(s_, yl_, c_), :], late.at[b, s], sem, device(ring, s_, yl_, c_))

        arrived(weights.at[pl.ds(0, 3)], weight_sem)

        def y_current(slots, q, k, plane):
            block = slots[q, k]
            grad = jnp.dot(block.reshape(bands * 32, 128), mat_y[...], preferred_element_type=F32)
            total = y_acc[plane]
            for n in range(bands):
                re, im = block[n, 0].astype(F32), block[n, 1].astype(F32)
                dre, dim = grad[32 * n : 32 * n + 16], grad[32 * n + 16 : 32 * n + 32]
                total = total + weights[q, n : n + 1, :] * (re * dim - im * dre)
            y_acc[plane] = total

        def groups(flips):
            return [2 * ((yl + j) % 2) + (c + i) % 2 for j, i in flips]

        order = groups(INNER_USE)

        for q in groups(OUTER_USE):
            arrived(outer.at[q], outer_sem.at[q])
            send(outer.at[q, 0], late.at[q, 2], edge_sem.at[q], below)
            send(outer.at[q, 1], late.at[q, 3], edge_sem.at[q], above)
            y_current(outer, q, 0, 0)
            y_current(outer, q, 1, 3)

        def to_owner(e, part, size):
            send(main_out.at[e, pl.ds(part, size)], main_in.at[s, pl.ds(part, size)], main_sem, device(ring, e, yo, co))

        near, far = 8.0 / 12.0, 1.0 / 12.0
        for e in range(2):
            main_out[e, 2] = far * y_acc[3 * e]
            to_owner(e, 2, 1)

        def term(u, v):
            return u[0] * v[1] - u[1] * v[0]

        names = [
            ("b1", "nxt"), ("b0", "nxt"), ("a1", "prv"), ("a1", "a0"), ("a1", "b0"), ("b0", "b1"), ("b0", "a0"), ("a1", "b1"),
        ]
        places = {"a0": (outer, 0), "b1": (outer, 1), "a1": (late, 0), "b0": (late, 1), "nxt": (late, 2), "prv": (late, 3)}

        def pair_sums(q, picked):
            def z_step(n, sums):
                w = weights[q, pl.ds(n, 1), :]
                used = sorted({name for p in picked for name in names[p]})
                field = {}
                for name in used:
                    slots, k = places[name]
                    field[name] = (slots[q, k, n, 0].astype(F32), slots[q, k, n, 1].astype(F32))
                scaled = {name: (w * field[name][0], w * field[name][1]) for name in sorted({names[p][0] for p in picked})}
                return tuple(x + term(scaled[names[p][0]], field[names[p][1]]) for x, p in zip(sums, picked))

            sums = lax.fori_loop(0, bands, z_step, tuple(pairs[p] for p in picked), unroll=4)
            for p, x in zip(picked, sums):
                pairs[p] = x

        @pl.when(relay_turn)
        def _():
            arrived(relay_in, relay_sem)
            start(*relay_copy())

        for j in range(1, 4):
            to = (b + j) % 4
            rows = pl.ds(pl.multiple_of(32 * to, 32), 32)
            send(x_acc.at[:, rows, :], x_in.at[b], x_sem, device(ring, s, to // 2, to % 2))

        def edge_up():
            extra_out[0] = near * pairs[0] - far * pairs[1]
            start(extra_out.at[0], extra_in.at[s], extra_sem, device(ring + 1, 0, yo, co))

        def edge_down():
            extra_out[1] = far * pairs[2]
            start(extra_out.at[1], extra_in.at[s], extra_sem, device(ring - 1, 1, yo, co))

        def inner_y(e):
            main_out[e, 3] = far * y_acc[1 + e]
            to_owner(e, 3, 1)

        for q in groups(SAME_USE):
            arrived(late.at[q, pl.ds(2, 2)], edge_sem.at[q])
            arrived(late.at[q, 0], same_sem.at[q])
            pl.when(s == 0)(lambda: pair_sums(q, (2,)))
            pl.when(s == 1)(lambda: pair_sums(q, (0, 1)))
            y_current(late, q, s, 1 + s)
        pl.when(s == 0)(edge_down)
        pl.when(s == 1)(edge_up)
        inner_y(s)

        for k, q in enumerate(order):
            arrived(late.at[q, 0], cross_sem.at[q])

            @pl.when(s == 1)
            def _():
                pair_sums(q, (2,))
                if k == 3:
                    edge_down()

            @pl.when((s == 0) & jnp.logical_not(ahead))
            def _():
                pair_sums(q, (0, 1))
                if k == 3:
                    edge_up()

            @pl.when((s == 0) & ahead)
            def _():
                pair_sums(q, (0, 1) if k < 3 else (1,))
                if k == 1:
                    pair_sums(order[3], (0,))
                if k == 2:
                    edge_up()

            pair_sums(q, range(3, 8))
            if k < 3:
                y_current(late, q, 1 - s, 2 - s)

        b1n0, b0n0, p1a1 = pairs[0], pairs[1], -pairs[2]
        a01, a1b0, b01, a0b0, a1b1 = -pairs[3], pairs[4], pairs[5], -pairs[6], pairs[7]
        main_out[0, 0] = near * a01 - far * a0b0
        main_out[0, 1] = near * (a1b0 + a01) - far * (a1b1 + p1a1)
        main_out[1, 0] = near * (b01 + a1b0) - far * (b0n0 + a0b0)
        main_out[1, 1] = near * (b1n0 + b01) - far * a1b1
        for e in range(2):
            to_owner(e, 0, 2)
        y_current(late, order[3], 1 - s, 2 - s)
        inner_y(1 - s)

        @pl.when(early & (s == 0))
        def _():
            q = order[3]
            arrived(tip_in, tip_sem)

            def step(n, total):
                w = weights[q, pl.ds(n, 1), :]
                here = [w * outer[q, 0, n, p].astype(F32) for p in range(2)]
                there = [tip_in[n, p].astype(F32) for p in range(2)]
                return total + term(there, here)

            extra_out[2] = -far * lax.fori_loop(0, bands, step, jnp.zeros((16, 128), F32), unroll=4)
            start(*sums_copy())

        arrived(x_in.at[pl.ds(0, 3)], x_sem)
        total = x_acc[:, pl.ds(pl.multiple_of(32 * b, 32), 32), :]
        for j in range(1, 4):
            total = total + x_in[(b + j) % 4]
        out[1] = total * far
        arrived(main_in, main_sem)
        arrived(extra_in, extra_sem)
        for h in range(2):
            rows = slice(16 * h, 16 * h + 16)
            out[0, :, rows, :] = main_in[h, :2]
            out[2, s, rows, :] = main_in[h, 2]
            out[2, 1 - s, rows, :] = main_in[h, 3]
            out[0, s, rows, :] += extra_in[h]

        @pl.when(early & (s == 0))
        def _():
            arrived(tip_sums, sums_sem)
            out[0, 0, :16, :] += tip_sums[...]

        def sent_copy(src, dst, sem, target):
            pltpu.make_async_remote_copy(
                src_ref=src, dst_ref=dst, send_sem=send_sem, recv_sem=sem, device_id=target, device_id_type=MESH
            ).wait_send()

        sent_copy(extra_out.at[0], extra_in.at[s], extra_sem, device(ring + 1, 0, yo, co))
        sent_copy(extra_out.at[1], extra_in.at[s], extra_sem, device(ring - 1, 1, yo, co))
        pl.when(early & (s == 0))(lambda: sent_copy(*sums_copy()))
        pl.when(tip_turn)(lambda: sent_copy(*tip_copy()))
        pl.when(relay_turn)(lambda: sent_copy(*relay_copy()))
        for copy in sent:
            copy.wait_send()

    return kernel


def solution(mesh):
    rings = mesh.shape["grid"] // 2

    def per_device(orbitals, occupations):
        n = orbitals.shape[0]
        dma = pltpu.SemaphoreType.DMA
        chunk = (n, 2, 16, 128)
        return pl.pallas_call(
            make_kernel(rings),
            out_shape=pltpu.VMEM((3, 2, 32, 128), F32),
            in_specs=[pl.BlockSpec(memory_space=pl.ANY), pl.BlockSpec(memory_space=pl.ANY)],
            out_specs=pl.BlockSpec(memory_space=pltpu.VMEM),
            scratch_shapes=[
                pltpu.SMEM((n,), F32),
                pltpu.VMEM((n, 2, 2, 128, 128), BF16),
                pltpu.VMEM((4, 2, *chunk), BF16),
                pltpu.VMEM((4, 4, *chunk), BF16),
                pltpu.VMEM((4, n, 128), F32),
                pltpu.VMEM((128, 128), BF16),
                pltpu.VMEM((128, 128), BF16),
                pltpu.VMEM((2, 128, 128), F32),
                pltpu.VMEM((4, 2, 32, 128), F32),
                pltpu.VMEM((4, 16, 128), F32),
                pltpu.VMEM((8, 16, 128), F32),
                pltpu.VMEM((2, 4, 16, 128), F32),
                pltpu.VMEM((2, 4, 16, 128), F32),
                pltpu.VMEM((3, 16, 128), F32),
                pltpu.VMEM((2, 16, 128), F32),
                pltpu.VMEM(chunk, BF16),
                pltpu.VMEM(chunk, BF16),
                pltpu.VMEM((16, 128), F32),
                dma, dma((2,)), dma, dma((4,)), dma((4,)), dma((4,)), dma((4,)), dma, dma, dma, dma, dma, dma, dma,
                pltpu.SemaphoreType.REGULAR, pltpu.SemaphoreType.REGULAR,
            ],
            compiler_params=pltpu.CompilerParams(collective_id=0, has_side_effects=True),
        )(orbitals, occupations)

    return jax.shard_map(
        per_device,
        mesh=mesh,
        in_specs=(P("band", None, "grid", None, None), P("band")),
        out_specs=P(None, "grid", "band", None),
        check_vma=False,
    )
```

```python
import jax
import jax.numpy as jnp
from jax import lax
from jax.experimental import pallas as pl
from jax.experimental.pallas import tpu as pltpu
from jax.sharding import PartitionSpec as P

MESH = pl.DeviceIdType.MESH
F32 = jnp.float32
BF16 = jnp.bfloat16


def stencil(n, transposed):
    i = lax.broadcasted_iota(jnp.int32, (n, n), 0)
    j = lax.broadcasted_iota(jnp.int32, (n, n), 1)
    d = (i - j if transposed else j - i) + n
    d = jnp.where(d >= n, d - n, d)
    near = jnp.where(d == 1, 8.0, 0.0) - jnp.where(d == n - 1, 8.0, 0.0)
    far = jnp.where(d == n - 2, 1.0, 0.0) - jnp.where(d == 2, 1.0, 0.0)
    return (near + far).astype(BF16)


OUTER = [(1, 0, 0), (1, 0, 1), (0, 0, 1), (0, 1, 0), (1, 1, 0), (0, 1, 1), (1, 1, 1)]
INNER = [(0, 0, 1), (0, 1, 0), (1, 1, 0), (0, 1, 1), (1, 1, 1), (1, 0, 0), (1, 0, 1)]
OUTER_USE = [(0, 0), (0, 1), (1, 0), (1, 1)]
INNER_USE = [(1, 0), (1, 1), (0, 0), (0, 1)]
SAME_USE = [(0, 0), (0, 1), (1, 0), (1, 1)]


def EARLY(ring, rings):
    return ring == 0, ring == rings - 1


def make_kernel(rings):
    def kernel(
        orb, occ_in, out,
        occ, own, outer, late, weights, mat_x, mat_y,
        x_acc, x_in, y_acc, pairs, main_out, main_in, extra_out, extra_in, tip_in, relay_in,
        occ_sem, load_sem, send_sem, outer_sem, edge_sem, same_sem, cross_sem, weight_sem, x_sem, main_sem, extra_sem, tip_sem, relay_sem,
        up_ready, down_ready,
    ):
        bands = own.shape[0]
        b = lax.axis_index("band")
        g = lax.axis_index("grid")
        ring, s = g // 2, g % 2
        yl, c = b // 2, b % 2
        def half(s_, yl_):
            return yl_ + s_ - 2 * s_ * yl_

        yo, co = half(s, yl), c
        turn = ring % 4

        def device(r, s_, yl_, c_):
            return {"band": 2 * yl_ + c_, "grid": 2 * ((r + rings) % rings) + s_}

        peers = [((s + i) % 2, (yl + j) % 2, (c + k) % 2) for i, j, k in OUTER]
        above, below = device(ring + 1, s, yl, c), device(ring - 1, s, yl, c)
        def my_rows(s_, yl_, c_):
            return pl.ds(pl.multiple_of(32 * (2 * half(s_, yl_) + c_) + 16 * s_, 16), 16)

        barrier = pltpu.get_barrier_semaphore()

        def signal(sem, target):
            pl.semaphore_signal(sem, inc=1, device_id=target, device_id_type=MESH)

        for s_, yl_, c_ in peers:
            signal(barrier, device(ring, s_, yl_, c_))
        pl.when(turn != 3)(lambda: signal(barrier, above))
        pl.when(turn == 0)(lambda: signal(barrier, below))
        early, ahead = EARLY(ring, rings)
        tip_turn, relay_turn = ahead & (s == 1), early & (s == 1)

        occ_load = pltpu.make_async_copy(occ_in, occ, occ_sem)
        loads = []
        for k, (plane, row, rows) in enumerate(((s, 64 * half(1 - s, yl), 64), (s, 64 * yo, 64), (1 - s, 0, 128))):
            at = pl.ds(pl.multiple_of(row, 64), rows)
            loads.append(pltpu.make_async_copy(orb.at[:, :, plane, at, :], own.at[:, :, plane, at, :], load_sem.at[k]))
        for load in (loads[0], loads[1], occ_load, loads[2]):
            load.start()

        mine = my_rows(s, yl, c)
        pltpu.make_async_copy(orb.at[:, :, s, mine, :], outer.at[b, s], outer_sem.at[b]).start()
        pltpu.make_async_copy(orb.at[:, :, 1 - s, mine, :], late.at[b, s], same_sem.at[b]).start()
        mat_x[...] = stencil(128, False)
        mat_y[...] = stencil(128, True)
        x_acc[...] = jnp.zeros_like(x_acc)
        y_acc[...] = jnp.zeros_like(y_acc)
        pairs[...] = jnp.zeros_like(pairs)
        occ_load.wait()
        for n in range(bands):
            weights[b, n : n + 1, :] = jnp.full((1, 128), occ[n], F32)
        loads[0].wait()
        pl.semaphore_wait(barrier, 7 + (turn + 1) // 2)

        def start(src, dst, sem, target):
            copy = pltpu.make_async_remote_copy(
                src_ref=src, dst_ref=dst, send_sem=send_sem, recv_sem=sem, device_id=target, device_id_type=MESH
            )
            copy.start()
            return copy

        sent = []

        def send(*args):
            sent.append(start(*args))

        def arrived(ref, sem):
            pltpu.make_async_copy(ref, ref, sem).wait()

        for j, i in [(0, 1), (1, 0), (1, 1)]:
            send(weights.at[b], weights.at[b], weight_sem, device(ring, s, (yl + j) % 2, (c + i) % 2))
        late_j, late_i = INNER_USE[3]
        yt, ct = (yl + late_j) % 2, (c + late_i) % 2

        def tip_copy():
            return (own.at[:, :, 0, my_rows(0, yt, ct), :], relay_in, relay_sem, above)

        def relay_copy():
            return (relay_in, tip_in, tip_sem, device(ring, 0, yt, ct))

        @pl.when(tip_turn)
        def _():
            loads[2].wait()
            start(*tip_copy())

        for k, (s_, yl_, c_) in enumerate(peers):
            if k == 2:
                loads[1].wait()
            send(own.at[:, :, s, my_rows(s_, yl_, c_), :], outer.at[b, s], outer_sem.at[b], device(ring, s_, yl_, c_))
        pl.when(turn != 0)(lambda: signal(up_ready, below))
        pl.when(turn == 3)(lambda: signal(down_ready, above))
        pl.when(jnp.logical_not(tip_turn))(lambda: loads[2].wait())

        def x_step(n, _):
            w = occ[n]
            for z in range(2):
                re = own[n, 0, z]
                im = own[n, 1, z]
                dre = jnp.dot(mat_x[...], re, preferred_element_type=F32)
                dim = jnp.dot(mat_x[...], im, preferred_element_type=F32)
                x_acc[z] += w * (re.astype(F32) * dim - im.astype(F32) * dre)
            return 0

        lax.fori_loop(0, bands, x_step, 0)

        pl.when(turn != 3)(lambda: pl.semaphore_wait(up_ready, 1))
        pl.when(turn == 0)(lambda: pl.semaphore_wait(down_ready, 1))
        for i, j, k in INNER:
            s_, yl_, c_ = (s + i) % 2, (yl + j) % 2, (c + k) % 2
            sem = (cross_sem if i else same_sem).at[b]
            send(own.at[:, :, 1 - s, my_rows(s_, yl_, c_), :], late.at[b, s], sem, device(ring, s_, yl_, c_))

        arrived(weights.at[pl.ds(0, 3)], weight_sem)

        def y_current(slots, q, k, plane):
            block = slots[q, k]
            grad = jnp.dot(block.reshape(bands * 32, 128), mat_y[...], preferred_element_type=F32)
            total = y_acc[plane]
            for n in range(bands):
                re, im = block[n, 0].astype(F32), block[n, 1].astype(F32)
                dre, dim = grad[32 * n : 32 * n + 16], grad[32 * n + 16 : 32 * n + 32]
                total = total + weights[q, n : n + 1, :] * (re * dim - im * dre)
            y_acc[plane] = total

        def groups(flips):
            return [2 * ((yl + j) % 2) + (c + i) % 2 for j, i in flips]

        order = groups(INNER_USE)

        for q in groups(OUTER_USE):
            arrived(outer.at[q], outer_sem.at[q])
            send(outer.at[q, 0], late.at[q, 2], edge_sem.at[q], below)
            send(outer.at[q, 1], late.at[q, 3], edge_sem.at[q], above)
            y_current(outer, q, 0, 0)
            y_current(outer, q, 1, 3)

        def main_copy(e, part, size):
            at = pl.ds(part, size)
            return (main_out.at[e, at], main_in.at[s, at], main_sem, device(ring, e, yo, co))

        def to_owner(e, part, size):
            if e == 1:
                start(*main_copy(e, part, size))
                return

            @pl.when(s == 1)
            def _():
                start(*main_copy(e, part, size))

            @pl.when(s == 0)
            def _():
                main_in[0, part : part + size] = main_out[0, part : part + size]

        near, far = 8.0 / 12.0, 1.0 / 12.0

        def term(u, v):
            return u[0] * v[1] - u[1] * v[0]

        names = [
            ("b1", "nxt"), ("b0", "nxt"), ("a1", "prv"), ("a1", "a0"), ("a1", "b0"), ("b0", "b1"), ("b0", "a0"), ("a1", "b1"),
        ]
        places = {"a0": (outer, 0), "b1": (outer, 1), "a1": (late, 0), "b0": (late, 1), "nxt": (late, 2), "prv": (late, 3)}

        def pair_sums(q, picked):
            def z_step(n, sums):
                w = weights[q, pl.ds(n, 1), :]
                used = sorted({name for p in picked for name in names[p]})
                field = {}
                for name in used:
                    slots, k = places[name]
                    field[name] = (slots[q, k, n, 0].astype(F32), slots[q, k, n, 1].astype(F32))
                scaled = {name: (w * field[name][0], w * field[name][1]) for name in sorted({names[p][0] for p in picked})}
                return tuple(x + term(scaled[names[p][0]], field[names[p][1]]) for x, p in zip(sums, picked))

            sums = lax.fori_loop(0, bands, z_step, tuple(pairs[p] for p in picked), unroll=4)
            for p, x in zip(picked, sums):
                pairs[p] = x

        @pl.when(relay_turn)
        def _():
            arrived(relay_in, relay_sem)
            start(*relay_copy())

        for j in range(1, 4):
            to = (b + j) % 4
            rows = pl.ds(pl.multiple_of(32 * to, 32), 32)
            send(x_acc.at[:, rows, :], x_in.at[b], x_sem, device(ring, s, to // 2, to % 2))

        for e in range(2):
            main_out[e, 2] = far * y_acc[3 * e]
            to_owner(e, 2, 1)

        def edge_up():
            extra_out[0] = near * pairs[0] - far * pairs[1]
            start(extra_out.at[0], extra_in.at[s], extra_sem, device(ring + 1, 0, yo, co))

        def edge_down():
            extra_out[1] = far * pairs[2]
            start(extra_out.at[1], extra_in.at[s], extra_sem, device(ring - 1, 1, yo, co))

        def inner_y(e):
            main_out[e, 3] = far * y_acc[1 + e]
            to_owner(e, 3, 1)

        for q in groups(SAME_USE):
            arrived(late.at[q, pl.ds(2, 2)], edge_sem.at[q])
            arrived(late.at[q, 0], same_sem.at[q])
            pl.when(s == 0)(lambda: pair_sums(q, (2,)))
            pl.when(s == 1)(lambda: pair_sums(q, (0, 1)))
            y_current(late, q, s, 1 + s)
        pl.when(s == 0)(edge_down)
        pl.when(s == 1)(edge_up)
        pl.when(s == 0)(lambda: inner_y(0))
        pl.when(s == 1)(lambda: inner_y(1))

        for k, q in enumerate(order):
            arrived(late.at[q, 0], cross_sem.at[q])

            @pl.when(s == 1)
            def _():
                pair_sums(q, (2,))
                if k == 3:
                    edge_down()

            @pl.when((s == 0) & jnp.logical_not(ahead))
            def _():
                pair_sums(q, (0, 1))
                if k == 3:
                    edge_up()

            @pl.when((s == 0) & ahead)
            def _():
                pair_sums(q, (0, 1) if k < 3 else (1,))
                if k == 1:
                    pair_sums(order[3], (0,))
                if k == 2:
                    edge_up()

            pair_sums(q, range(3, 8))
            if k < 3:
                y_current(late, q, 1 - s, 2 - s)

        b1n0, b0n0, p1a1 = pairs[0], pairs[1], -pairs[2]
        a01, a1b0, b01, a0b0, a1b1 = -pairs[3], pairs[4], pairs[5], -pairs[6], pairs[7]
        main_out[0, 0] = near * a01 - far * a0b0
        main_out[0, 1] = near * (a1b0 + a01) - far * (a1b1 + p1a1)
        main_out[1, 0] = near * (b01 + a1b0) - far * (b0n0 + a0b0)
        main_out[1, 1] = near * (b1n0 + b01) - far * a1b1
        for e in range(2):
            to_owner(e, 0, 2)
        y_current(late, order[3], 1 - s, 2 - s)
        pl.when(s == 0)(lambda: inner_y(1))
        pl.when(s == 1)(lambda: inner_y(0))

        arrived(x_in.at[pl.ds(0, 3)], x_sem)
        total = x_acc[:, pl.ds(pl.multiple_of(32 * b, 32), 32), :]
        for j in range(1, 4):
            total = total + x_in[(b + j) % 4]
        out[1] = total * far
        @pl.when(early & (s == 0))
        def _():
            q = order[3]
            arrived(tip_in, tip_sem)

            def step(n, total):
                w = weights[q, pl.ds(n, 1), :]
                here = [w * outer[q, 0, n, p].astype(F32) for p in range(2)]
                there = [tip_in[n, p].astype(F32) for p in range(2)]
                return total + term(there, here)

            main_in[0, 0] -= far * lax.fori_loop(0, bands, step, jnp.zeros((16, 128), F32), unroll=4)

        pl.when(s == 0)(lambda: arrived(main_in.at[1], main_sem))
        pl.when(s == 1)(lambda: arrived(main_in, main_sem))
        arrived(extra_in, extra_sem)
        for h in range(2):
            rows = slice(16 * h, 16 * h + 16)
            out[0, :, rows, :] = main_in[h, :2]
            out[2, s, rows, :] = main_in[h, 2]
            out[2, 1 - s, rows, :] = main_in[h, 3]
            out[0, s, rows, :] += extra_in[h]

        def sent_copy(src, dst, sem, target):
            pltpu.make_async_remote_copy(
                src_ref=src, dst_ref=dst, send_sem=send_sem, recv_sem=sem, device_id=target, device_id_type=MESH
            ).wait_send()

        sent_copy(extra_out.at[0], extra_in.at[s], extra_sem, device(ring + 1, 0, yo, co))
        sent_copy(extra_out.at[1], extra_in.at[s], extra_sem, device(ring - 1, 1, yo, co))
        for part, size in ((0, 2), (2, 1), (3, 1)):
            sent_copy(*main_copy(1, part, size))

        @pl.when(s == 1)
        def _():
            for part, size in ((0, 2), (2, 1), (3, 1)):
                sent_copy(*main_copy(0, part, size))

        pl.when(tip_turn)(lambda: sent_copy(*tip_copy()))
        pl.when(relay_turn)(lambda: sent_copy(*relay_copy()))
        for copy in sent:
            copy.wait_send()

    return kernel


def solution(mesh):
    rings = mesh.shape["grid"] // 2

    def per_device(orbitals, occupations):
        n = orbitals.shape[0]
        dma = pltpu.SemaphoreType.DMA
        chunk = (n, 2, 16, 128)
        return pl.pallas_call(
            make_kernel(rings),
            out_shape=pltpu.VMEM((3, 2, 32, 128), F32),
            in_specs=[pl.BlockSpec(memory_space=pl.ANY), pl.BlockSpec(memory_space=pl.ANY)],
            out_specs=pl.BlockSpec(memory_space=pltpu.VMEM),
            scratch_shapes=[
                pltpu.SMEM((n,), F32),
                pltpu.VMEM((n, 2, 2, 128, 128), BF16),
                pltpu.VMEM((4, 2, *chunk), BF16),
                pltpu.VMEM((4, 4, *chunk), BF16),
                pltpu.VMEM((4, n, 128), F32),
                pltpu.VMEM((128, 128), BF16),
                pltpu.VMEM((128, 128), BF16),
                pltpu.VMEM((2, 128, 128), F32),
                pltpu.VMEM((4, 2, 32, 128), F32),
                pltpu.VMEM((4, 16, 128), F32),
                pltpu.VMEM((8, 16, 128), F32),
                pltpu.VMEM((2, 4, 16, 128), F32),
                pltpu.VMEM((2, 4, 16, 128), F32),
                pltpu.VMEM((2, 16, 128), F32),
                pltpu.VMEM((2, 16, 128), F32),
                pltpu.VMEM(chunk, BF16),
                pltpu.VMEM(chunk, BF16),
                dma, dma((3,)), dma, dma((4,)), dma((4,)), dma((4,)), dma((4,)), dma, dma, dma, dma, dma, dma,
                pltpu.SemaphoreType.REGULAR, pltpu.SemaphoreType.REGULAR,
            ],
            compiler_params=pltpu.CompilerParams(collective_id=0, has_side_effects=True),
        )(orbitals, occupations)

    return jax.shard_map(
        per_device,
        mesh=mesh,
        in_specs=(P("band", None, "grid", None, None), P("band")),
        out_specs=P(None, "grid", "band", None),
        check_vma=False,
    )
```

```python
import jax
import jax.numpy as jnp
from jax import lax
from jax.experimental import pallas as pl
from jax.experimental.pallas import tpu as pltpu
from jax.sharding import PartitionSpec as P

MESH = pl.DeviceIdType.MESH
F32 = jnp.float32
BF16 = jnp.bfloat16


def stencil(n, transposed):
    i = lax.broadcasted_iota(jnp.int32, (n, n), 0)
    j = lax.broadcasted_iota(jnp.int32, (n, n), 1)
    d = (i - j if transposed else j - i) + n
    d = jnp.where(d >= n, d - n, d)
    near = jnp.where(d == 1, 8.0, 0.0) - jnp.where(d == n - 1, 8.0, 0.0)
    far = jnp.where(d == n - 2, 1.0, 0.0) - jnp.where(d == 2, 1.0, 0.0)
    return (near + far).astype(BF16)


OUTER = [(1, 0, 0), (1, 0, 1), (0, 0, 1), (0, 1, 0), (1, 1, 0), (0, 1, 1), (1, 1, 1)]
INNER = [(0, 0, 1), (0, 1, 0), (1, 1, 0), (0, 1, 1), (1, 1, 1), (1, 0, 0), (1, 0, 1)]
OUTER_USE = [(0, 0), (0, 1), (1, 0), (1, 1)]
INNER_USE = [(1, 0), (1, 1), (0, 0), (0, 1)]
SAME_USE = [(0, 0), (0, 1), (1, 0), (1, 1)]


def EARLY(ring, rings):
    return ring % 4 == 0, ring % 4 == 3


def make_kernel(rings):
    def kernel(
        orb, occ_in, out,
        occ, own, outer, late, weights, mat_x, mat_y,
        x_acc, x_in, y_acc, pairs, main_out, main_in, extra_out, extra_in, tip_in, relay_in, tip_two, relay_two,
        occ_sem, load_sem, send_sem, outer_sem, edge_sem, same_sem, cross_sem, weight_sem, x_sem, main_sem, extra_sem, tip_sem, relay_sem, tip_two_sem, relay_two_sem,
        up_ready, down_ready,
    ):
        bands = own.shape[0]
        b = lax.axis_index("band")
        g = lax.axis_index("grid")
        ring, s = g // 2, g % 2
        yl, c = b // 2, b % 2
        def half(s_, yl_):
            return yl_ + s_ - 2 * s_ * yl_

        yo, co = half(s, yl), c
        turn = ring % 4

        def device(r, s_, yl_, c_):
            return {"band": 2 * yl_ + c_, "grid": 2 * ((r + rings) % rings) + s_}

        peers = [((s + i) % 2, (yl + j) % 2, (c + k) % 2) for i, j, k in OUTER]
        above, below = device(ring + 1, s, yl, c), device(ring - 1, s, yl, c)
        def my_rows(s_, yl_, c_):
            return pl.ds(pl.multiple_of(32 * (2 * half(s_, yl_) + c_) + 16 * s_, 16), 16)

        barrier = pltpu.get_barrier_semaphore()

        def signal(sem, target):
            pl.semaphore_signal(sem, inc=1, device_id=target, device_id_type=MESH)

        for s_, yl_, c_ in peers:
            signal(barrier, device(ring, s_, yl_, c_))
        pl.when(turn != 3)(lambda: signal(barrier, above))
        pl.when(turn == 0)(lambda: signal(barrier, below))
        early, ahead = EARLY(ring, rings)
        tip_turn, relay_turn = ahead & (s == 1), early & (s == 1)
        first, last = (ring == 0) & (c == 0), (ring == rings - 1) & (c == 0)

        occ_load = pltpu.make_async_copy(occ_in, occ, occ_sem)
        loads = []
        for k, (plane, row, rows) in enumerate(((s, 64 * half(1 - s, yl), 64), (s, 64 * yo, 64), (1 - s, 0, 128))):
            at = pl.ds(pl.multiple_of(row, 64), rows)
            loads.append(pltpu.make_async_copy(orb.at[:, :, plane, at, :], own.at[:, :, plane, at, :], load_sem.at[k]))
        for load in (loads[0], loads[1], occ_load, loads[2]):
            load.start()

        mine = my_rows(s, yl, c)
        pltpu.make_async_copy(orb.at[:, :, s, mine, :], outer.at[b, s], outer_sem.at[b]).start()
        pltpu.make_async_copy(orb.at[:, :, 1 - s, mine, :], late.at[b, s], same_sem.at[b]).start()
        mat_x[...] = stencil(128, False)
        mat_y[...] = stencil(128, True)
        x_acc[...] = jnp.zeros_like(x_acc)
        y_acc[...] = jnp.zeros_like(y_acc)
        pairs[...] = jnp.zeros_like(pairs)
        occ_load.wait()
        for n in range(bands):
            weights[b, n : n + 1, :] = jnp.full((1, 128), occ[n], F32)
        loads[0].wait()
        pl.semaphore_wait(barrier, 7 + (turn + 1) // 2)

        def start(src, dst, sem, target):
            copy = pltpu.make_async_remote_copy(
                src_ref=src, dst_ref=dst, send_sem=send_sem, recv_sem=sem, device_id=target, device_id_type=MESH
            )
            copy.start()
            return copy

        sent = []

        def send(*args):
            sent.append(start(*args))

        def arrived(ref, sem):
            pltpu.make_async_copy(ref, ref, sem).wait()

        for j, i in [(0, 1), (1, 0), (1, 1)]:
            send(weights.at[b], weights.at[b], weight_sem, device(ring, s, (yl + j) % 2, (c + i) % 2))
        late_j, late_i = INNER_USE[3]
        yt, ct = (yl + late_j) % 2, (c + late_i) % 2

        def tip_copy():
            return (own.at[:, :, 0, my_rows(0, yt, ct), :], relay_in, relay_sem, above)

        def tip_two_copy():
            return (own.at[:, :, 0, my_rows(0, yl, c), :], relay_two, relay_two_sem, above)

        def relay_two_copy():
            return (relay_two, tip_two, tip_two_sem, device(ring, 0, yl, c))

        def relay_copy():
            return (relay_in, tip_in, tip_sem, device(ring, 0, yt, ct))

        @pl.when(tip_turn)
        def _():
            loads[2].wait()
            start(*tip_copy())

            @pl.when(last)
            def _():
                start(*tip_two_copy())

        for k, (s_, yl_, c_) in enumerate(peers):
            if k == 2:
                loads[1].wait()
            send(own.at[:, :, s, my_rows(s_, yl_, c_), :], outer.at[b, s], outer_sem.at[b], device(ring, s_, yl_, c_))
        pl.when(turn != 0)(lambda: signal(up_ready, below))
        pl.when(turn == 3)(lambda: signal(down_ready, above))
        pl.when(jnp.logical_not(tip_turn))(lambda: loads[2].wait())

        def x_step(n, _):
            w = occ[n]
            for z in range(2):
                re = own[n, 0, z]
                im = own[n, 1, z]
                dre = jnp.dot(mat_x[...], re, preferred_element_type=F32)
                dim = jnp.dot(mat_x[...], im, preferred_element_type=F32)
                x_acc[z] += w * (re.astype(F32) * dim - im.astype(F32) * dre)
            return 0

        lax.fori_loop(0, bands, x_step, 0)

        pl.when(turn != 3)(lambda: pl.semaphore_wait(up_ready, 1))
        pl.when(turn == 0)(lambda: pl.semaphore_wait(down_ready, 1))
        for i, j, k in INNER:
            s_, yl_, c_ = (s + i) % 2, (yl + j) % 2, (c + k) % 2
            sem = (cross_sem if i else same_sem).at[b]
            send(own.at[:, :, 1 - s, my_rows(s_, yl_, c_), :], late.at[b, s], sem, device(ring, s_, yl_, c_))

        arrived(weights.at[pl.ds(0, 3)], weight_sem)

        def y_current(slots, q, k, plane):
            block = slots[q, k]
            grad = jnp.dot(block.reshape(bands * 32, 128), mat_y[...], preferred_element_type=F32)
            total = y_acc[plane]
            for n in range(bands):
                re, im = block[n, 0].astype(F32), block[n, 1].astype(F32)
                dre, dim = grad[32 * n : 32 * n + 16], grad[32 * n + 16 : 32 * n + 32]
                total = total + weights[q, n : n + 1, :] * (re * dim - im * dre)
            y_acc[plane] = total

        def groups(flips):
            return [2 * ((yl + j) % 2) + (c + i) % 2 for j, i in flips]

        order = groups(INNER_USE)

        for q in groups(OUTER_USE):
            arrived(outer.at[q], outer_sem.at[q])
            send(outer.at[q, 0], late.at[q, 2], edge_sem.at[q], below)
            send(outer.at[q, 1], late.at[q, 3], edge_sem.at[q], above)
            y_current(outer, q, 0, 0)
            y_current(outer, q, 1, 3)

        def main_copy(e, part, size):
            at = pl.ds(part, size)
            return (main_out.at[e, at], main_in.at[s, at], main_sem, device(ring, e, yo, co))

        def to_owner(e, part, size):
            if e == 1:
                start(*main_copy(e, part, size))
                return

            @pl.when(s == 1)
            def _():
                start(*main_copy(e, part, size))

            @pl.when(s == 0)
            def _():
                main_in[0, part : part + size] = main_out[0, part : part + size]

        near, far = 8.0 / 12.0, 1.0 / 12.0

        def term(u, v):
            return u[0] * v[1] - u[1] * v[0]

        names = [
            ("b1", "nxt"), ("b0", "nxt"), ("a1", "prv"), ("a1", "a0"), ("a1", "b0"), ("b0", "b1"), ("b0", "a0"), ("a1", "b1"),
        ]
        places = {"a0": (outer, 0), "b1": (outer, 1), "a1": (late, 0), "b0": (late, 1), "nxt": (late, 2), "prv": (late, 3)}

        def pair_sums(q, picked):
            def z_step(n, sums):
                w = weights[q, pl.ds(n, 1), :]
                used = sorted({name for p in picked for name in names[p]})
                field = {}
                for name in used:
                    slots, k = places[name]
                    field[name] = (slots[q, k, n, 0].astype(F32), slots[q, k, n, 1].astype(F32))
                scaled = {name: (w * field[name][0], w * field[name][1]) for name in sorted({names[p][0] for p in picked})}
                return tuple(x + term(scaled[names[p][0]], field[names[p][1]]) for x, p in zip(sums, picked))

            sums = lax.fori_loop(0, bands, z_step, tuple(pairs[p] for p in picked), unroll=4)
            for p, x in zip(picked, sums):
                pairs[p] = x

        @pl.when(relay_turn)
        def _():
            arrived(relay_in, relay_sem)
            start(*relay_copy())

            @pl.when(first)
            def _():
                arrived(relay_two, relay_two_sem)
                start(*relay_two_copy())

        for j in range(1, 4):
            to = (b + j) % 4
            rows = pl.ds(pl.multiple_of(32 * to, 32), 32)
            send(x_acc.at[:, rows, :], x_in.at[b], x_sem, device(ring, s, to // 2, to % 2))

        for e in range(2):
            main_out[e, 2] = far * y_acc[3 * e]
            to_owner(e, 2, 1)

        def edge_up():
            extra_out[0] = near * pairs[0] - far * pairs[1]
            start(extra_out.at[0], extra_in.at[s], extra_sem, device(ring + 1, 0, yo, co))

        def edge_down():
            extra_out[1] = far * pairs[2]
            start(extra_out.at[1], extra_in.at[s], extra_sem, device(ring - 1, 1, yo, co))

        def inner_y(e):
            main_out[e, 3] = far * y_acc[1 + e]
            to_owner(e, 3, 1)

        for q in groups(SAME_USE):
            arrived(late.at[q, pl.ds(2, 2)], edge_sem.at[q])
            arrived(late.at[q, 0], same_sem.at[q])
            pl.when(s == 0)(lambda: pair_sums(q, (2,)))
            pl.when(s == 1)(lambda: pair_sums(q, (0, 1)))
            y_current(late, q, s, 1 + s)
        pl.when(s == 0)(edge_down)
        pl.when(s == 1)(edge_up)
        pl.when(s == 0)(lambda: inner_y(0))
        pl.when(s == 1)(lambda: inner_y(1))

        for k, q in enumerate(order):
            arrived(late.at[q, 0], cross_sem.at[q])

            @pl.when(s == 1)
            def _():
                pair_sums(q, (2,))
                if k == 3:
                    edge_down()

            @pl.when((s == 0) & jnp.logical_not(ahead))
            def _():
                pair_sums(q, (0, 1))
                if k == 3:
                    edge_up()

            @pl.when((s == 0) & ahead)
            def _():
                pair_sums(q, (0, 1) if k < 2 else (1,))
                if k == 1:
                    pair_sums(order[2], (0,))
                    pair_sums(order[3], (0,))
                    pl.when(last)(edge_up)
                if k == 2:
                    pl.when(jnp.logical_not(last))(edge_up)

            pair_sums(q, range(3, 8))
            if k < 3:
                y_current(late, q, 1 - s, 2 - s)

        b1n0, b0n0, p1a1 = pairs[0], pairs[1], -pairs[2]
        a01, a1b0, b01, a0b0, a1b1 = -pairs[3], pairs[4], pairs[5], -pairs[6], pairs[7]
        main_out[0, 0] = near * a01 - far * a0b0
        main_out[0, 1] = near * (a1b0 + a01) - far * (a1b1 + p1a1)
        main_out[1, 0] = near * (b01 + a1b0) - far * (b0n0 + a0b0)
        main_out[1, 1] = near * (b1n0 + b01) - far * a1b1
        for e in range(2):
            to_owner(e, 0, 2)
        y_current(late, order[3], 1 - s, 2 - s)
        pl.when(s == 0)(lambda: inner_y(1))
        pl.when(s == 1)(lambda: inner_y(0))

        arrived(x_in.at[pl.ds(0, 3)], x_sem)
        total = x_acc[:, pl.ds(pl.multiple_of(32 * b, 32), 32), :]
        for j in range(1, 4):
            total = total + x_in[(b + j) % 4]
        out[1] = total * far
        def tip_current(q, tip, sem):
            arrived(tip, sem)

            def step(n, total):
                w = weights[q, pl.ds(n, 1), :]
                here = [w * outer[q, 0, n, p].astype(F32) for p in range(2)]
                there = [tip[n, p].astype(F32) for p in range(2)]
                return total + term(there, here)

            main_in[0, 0] -= far * lax.fori_loop(0, bands, step, jnp.zeros((16, 128), F32), unroll=4)

        pl.when(early & (s == 0))(lambda: tip_current(order[3], tip_in, tip_sem))
        pl.when(first & (s == 0))(lambda: tip_current(order[2], tip_two, tip_two_sem))
        pl.when(s == 0)(lambda: arrived(main_in.at[1], main_sem))
        pl.when(s == 1)(lambda: arrived(main_in, main_sem))
        for h in range(2):
            rows = slice(16 * h, 16 * h + 16)
            out[0, :, rows, :] = main_in[h, :2]
            out[2, s, rows, :] = main_in[h, 2]
            out[2, 1 - s, rows, :] = main_in[h, 3]

        def sent_copy(src, dst, sem, target):
            pltpu.make_async_remote_copy(
                src_ref=src, dst_ref=dst, send_sem=send_sem, recv_sem=sem, device_id=target, device_id_type=MESH
            ).wait_send()

        sent_copy(extra_out.at[0], extra_in.at[s], extra_sem, device(ring + 1, 0, yo, co))
        sent_copy(extra_out.at[1], extra_in.at[s], extra_sem, device(ring - 1, 1, yo, co))
        for part, size in ((0, 2), (2, 1), (3, 1)):
            sent_copy(*main_copy(1, part, size))

        @pl.when(s == 1)
        def _():
            for part, size in ((0, 2), (2, 1), (3, 1)):
                sent_copy(*main_copy(0, part, size))

        pl.when(tip_turn)(lambda: sent_copy(*tip_copy()))
        pl.when(relay_turn)(lambda: sent_copy(*relay_copy()))
        pl.when(tip_turn & last)(lambda: sent_copy(*tip_two_copy()))
        pl.when(relay_turn & first)(lambda: sent_copy(*relay_two_copy()))
        for copy in sent:
            copy.wait_send()

        arrived(extra_in, extra_sem)
        for h in range(2):
            out[0, s, 16 * h : 16 * h + 16, :] += extra_in[h]

    return kernel


def solution(mesh):
    rings = mesh.shape["grid"] // 2

    def per_device(orbitals, occupations):
        n = orbitals.shape[0]
        dma = pltpu.SemaphoreType.DMA
        chunk = (n, 2, 16, 128)
        return pl.pallas_call(
            make_kernel(rings),
            out_shape=pltpu.VMEM((3, 2, 32, 128), F32),
            in_specs=[pl.BlockSpec(memory_space=pl.ANY), pl.BlockSpec(memory_space=pl.ANY)],
            out_specs=pl.BlockSpec(memory_space=pltpu.VMEM),
            scratch_shapes=[
                pltpu.SMEM((n,), F32),
                pltpu.VMEM((n, 2, 2, 128, 128), BF16),
                pltpu.VMEM((4, 2, *chunk), BF16),
                pltpu.VMEM((4, 4, *chunk), BF16),
                pltpu.VMEM((4, n, 128), F32),
                pltpu.VMEM((128, 128), BF16),
                pltpu.VMEM((128, 128), BF16),
                pltpu.VMEM((2, 128, 128), F32),
                pltpu.VMEM((4, 2, 32, 128), F32),
                pltpu.VMEM((4, 16, 128), F32),
                pltpu.VMEM((8, 16, 128), F32),
                pltpu.VMEM((2, 4, 16, 128), F32),
                pltpu.VMEM((2, 4, 16, 128), F32),
                pltpu.VMEM((2, 16, 128), F32),
                pltpu.VMEM((2, 16, 128), F32),
                pltpu.VMEM(chunk, BF16),
                pltpu.VMEM(chunk, BF16),
                pltpu.VMEM(chunk, BF16),
                pltpu.VMEM(chunk, BF16),
                dma, dma((3,)), dma, dma((4,)), dma((4,)), dma((4,)), dma((4,)), dma, dma, dma, dma, dma, dma, dma, dma,
                pltpu.SemaphoreType.REGULAR, pltpu.SemaphoreType.REGULAR,
            ],
            compiler_params=pltpu.CompilerParams(collective_id=0, has_side_effects=True),
        )(orbitals, occupations)

    return jax.shard_map(
        per_device,
        mesh=mesh,
        in_specs=(P("band", None, "grid", None, None), P("band")),
        out_specs=P(None, "grid", "band", None),
        check_vma=False,
    )
```

```python
import jax
import jax.numpy as jnp
from jax import lax
from jax.experimental import pallas as pl
from jax.experimental.pallas import tpu as pltpu
from jax.sharding import PartitionSpec as P

MESH = pl.DeviceIdType.MESH
F32 = jnp.float32
BF16 = jnp.bfloat16


def stencil(n, transposed):
    i = lax.broadcasted_iota(jnp.int32, (n, n), 0)
    j = lax.broadcasted_iota(jnp.int32, (n, n), 1)
    d = (i - j if transposed else j - i) + n
    d = jnp.where(d >= n, d - n, d)
    near = jnp.where(d == 1, 8.0, 0.0) - jnp.where(d == n - 1, 8.0, 0.0)
    far = jnp.where(d == n - 2, 1.0, 0.0) - jnp.where(d == 2, 1.0, 0.0)
    return (near + far).astype(BF16)


OUTER = [(1, 0, 0), (1, 0, 1), (0, 0, 1), (0, 1, 0), (1, 1, 0), (0, 1, 1), (1, 1, 1)]
INNER = [(0, 0, 1), (0, 1, 0), (1, 1, 0), (0, 1, 1), (1, 1, 1), (1, 0, 0), (1, 0, 1)]
OUTER_USE = [(0, 0), (0, 1), (1, 0), (1, 1)]
INNER_USE = [(1, 0), (1, 1), (0, 0), (0, 1)]
SAME_USE = [(0, 0), (0, 1), (1, 0), (1, 1)]


def EARLY(ring, rings):
    return ring % 4 == 0, ring % 4 == 3


def make_kernel(rings):
    def kernel(
        orb, occ_in, out,
        occ, own, outer, late, weights, mat_x, mat_y,
        x_acc, x_in, y_acc, pairs, main_out, main_in, extra_out, extra_in, tip_in, relay_in, tip_two, relay_two,
        occ_sem, load_sem, send_sem, outer_sem, edge_sem, same_sem, cross_sem, weight_sem, x_sem, main_sem, extra_sem, tip_sem, relay_sem, tip_two_sem, relay_two_sem,
        up_ready, down_ready,
    ):
        bands = own.shape[0]
        b = lax.axis_index("band")
        g = lax.axis_index("grid")
        ring, s = g // 2, g % 2
        yl, c = b // 2, b % 2
        def half(s_, yl_):
            return yl_ + s_ - 2 * s_ * yl_

        yo, co = half(s, yl), c
        turn = ring % 4

        def device(r, s_, yl_, c_):
            return {"band": 2 * yl_ + c_, "grid": 2 * ((r + rings) % rings) + s_}

        peers = [((s + i) % 2, (yl + j) % 2, (c + k) % 2) for i, j, k in OUTER]
        above, below = device(ring + 1, s, yl, c), device(ring - 1, s, yl, c)
        def my_rows(s_, yl_, c_):
            return pl.ds(pl.multiple_of(32 * (2 * half(s_, yl_) + c_) + 16 * s_, 16), 16)

        barrier = pltpu.get_barrier_semaphore()

        def signal(sem, target):
            pl.semaphore_signal(sem, inc=1, device_id=target, device_id_type=MESH)

        for s_, yl_, c_ in peers:
            signal(barrier, device(ring, s_, yl_, c_))
        pl.when(turn != 3)(lambda: signal(barrier, above))
        pl.when(turn == 0)(lambda: signal(barrier, below))
        early, ahead = EARLY(ring, rings)
        tip_turn, relay_turn = ahead & (s == 1), early & (s == 1)
        first, last = (ring == 0) & (c == 0), (ring == rings - 1) & (c == 0)

        occ_load = pltpu.make_async_copy(occ_in, occ, occ_sem)
        loads = []
        for k, (plane, row, rows) in enumerate(((s, 64 * half(1 - s, yl), 64), (s, 64 * yo, 64), (1 - s, 0, 128))):
            at = pl.ds(pl.multiple_of(row, 64), rows)
            loads.append(pltpu.make_async_copy(orb.at[:, :, plane, at, :], own.at[:, :, plane, at, :], load_sem.at[k]))
        for load in (loads[0], loads[1], occ_load, loads[2]):
            load.start()

        mine = my_rows(s, yl, c)
        pltpu.make_async_copy(orb.at[:, :, s, mine, :], outer.at[b, s], outer_sem.at[b]).start()
        pltpu.make_async_copy(orb.at[:, :, 1 - s, mine, :], late.at[b, s], same_sem.at[b]).start()
        mat_x[...] = stencil(128, False)
        mat_y[...] = stencil(128, True)
        x_acc[...] = jnp.zeros_like(x_acc)
        y_acc[...] = jnp.zeros_like(y_acc)
        pairs[...] = jnp.zeros_like(pairs)
        occ_load.wait()
        for n in range(bands):
            weights[b, n : n + 1, :] = jnp.full((1, 128), occ[n], F32)
        loads[0].wait()
        pl.semaphore_wait(barrier, 7 + (turn + 1) // 2)

        def start(src, dst, sem, target):
            copy = pltpu.make_async_remote_copy(
                src_ref=src, dst_ref=dst, send_sem=send_sem, recv_sem=sem, device_id=target, device_id_type=MESH
            )
            copy.start()
            return copy

        sent = []

        def send(*args):
            sent.append(start(*args))

        def arrived(ref, sem):
            pltpu.make_async_copy(ref, ref, sem).wait()

        for j, i in [(0, 1), (1, 0), (1, 1)]:
            send(weights.at[b], weights.at[b], weight_sem, device(ring, s, (yl + j) % 2, (c + i) % 2))
        late_j, late_i = INNER_USE[3]
        yt, ct = (yl + late_j) % 2, (c + late_i) % 2

        def tip_copy():
            return (own.at[:, :, 0, my_rows(0, yt, ct), :], relay_in, relay_sem, above)

        def tip_two_copy():
            return (own.at[:, :, 0, my_rows(0, yl, c), :], relay_two, relay_two_sem, above)

        def relay_two_copy():
            return (relay_two, tip_two, tip_two_sem, device(ring, 0, yl, c))

        def relay_copy():
            return (relay_in, tip_in, tip_sem, device(ring, 0, yt, ct))

        @pl.when(tip_turn)
        def _():
            loads[2].wait()
            start(*tip_copy())

            @pl.when(last)
            def _():
                start(*tip_two_copy())

        for k, (s_, yl_, c_) in enumerate(peers):
            if k == 2:
                loads[1].wait()
            send(own.at[:, :, s, my_rows(s_, yl_, c_), :], outer.at[b, s], outer_sem.at[b], device(ring, s_, yl_, c_))
        pl.when(turn != 0)(lambda: signal(up_ready, below))
        pl.when(turn == 3)(lambda: signal(down_ready, above))
        pl.when(jnp.logical_not(tip_turn))(lambda: loads[2].wait())

        def x_step(n, _):
            w = occ[n]
            for z in range(2):
                re = own[n, 0, z]
                im = own[n, 1, z]
                dre = jnp.dot(mat_x[...], re, preferred_element_type=F32)
                dim = jnp.dot(mat_x[...], im, preferred_element_type=F32)
                x_acc[z] += w * (re.astype(F32) * dim - im.astype(F32) * dre)
            return 0

        lax.fori_loop(0, bands, x_step, 0)

        pl.when(turn != 3)(lambda: pl.semaphore_wait(up_ready, 1))
        pl.when(turn == 0)(lambda: pl.semaphore_wait(down_ready, 1))
        for i, j, k in INNER:
            s_, yl_, c_ = (s + i) % 2, (yl + j) % 2, (c + k) % 2
            sem = (cross_sem if i else same_sem).at[b]
            send(own.at[:, :, 1 - s, my_rows(s_, yl_, c_), :], late.at[b, s], sem, device(ring, s_, yl_, c_))

        arrived(weights.at[pl.ds(0, 3)], weight_sem)

        def y_current(slots, q, k, plane):
            block = slots[q, k]
            grad = jnp.dot(block.reshape(bands * 32, 128), mat_y[...], preferred_element_type=F32)
            total = y_acc[plane]
            for n in range(bands):
                re, im = block[n, 0].astype(F32), block[n, 1].astype(F32)
                dre, dim = grad[32 * n : 32 * n + 16], grad[32 * n + 16 : 32 * n + 32]
                total = total + weights[q, n : n + 1, :] * (re * dim - im * dre)
            y_acc[plane] = total

        def groups(flips):
            return [2 * ((yl + j) % 2) + (c + i) % 2 for j, i in flips]

        order = groups(INNER_USE)

        for q in groups(OUTER_USE):
            arrived(outer.at[q], outer_sem.at[q])
            send(outer.at[q, 0], late.at[q, 2], edge_sem.at[q], below)
            send(outer.at[q, 1], late.at[q, 3], edge_sem.at[q], above)
            y_current(outer, q, 0, 0)
            y_current(outer, q, 1, 3)

        def main_copy(e, part, size):
            at = pl.ds(part, size)
            return (main_out.at[e, at], main_in.at[s, at], main_sem, device(ring, e, yo, co))

        def to_owner(e, part, size):
            if e == 1:
                start(*main_copy(e, part, size))
                return

            @pl.when(s == 1)
            def _():
                start(*main_copy(e, part, size))

            @pl.when(s == 0)
            def _():
                main_in[0, part : part + size] = main_out[0, part : part + size]

        near, far = 8.0 / 12.0, 1.0 / 12.0

        def term(u, v):
            return u[0] * v[1] - u[1] * v[0]

        names = [
            ("b1", "nxt"), ("b0", "nxt"), ("a1", "prv"), ("a1", "a0"), ("a1", "b0"), ("b0", "b1"), ("b0", "a0"), ("a1", "b1"),
        ]
        places = {"a0": (outer, 0), "b1": (outer, 1), "a1": (late, 0), "b0": (late, 1), "nxt": (late, 2), "prv": (late, 3)}

        def pair_sums(q, picked):
            def z_step(n, sums):
                w = weights[q, pl.ds(n, 1), :]
                used = sorted({name for p in picked for name in names[p]})
                field = {}
                for name in used:
                    slots, k = places[name]
                    field[name] = (slots[q, k, n, 0].astype(F32), slots[q, k, n, 1].astype(F32))
                scaled = {name: (w * field[name][0], w * field[name][1]) for name in sorted({names[p][0] for p in picked})}
                return tuple(x + term(scaled[names[p][0]], field[names[p][1]]) for x, p in zip(sums, picked))

            sums = lax.fori_loop(0, bands, z_step, tuple(pairs[p] for p in picked), unroll=8)
            for p, x in zip(picked, sums):
                pairs[p] = x

        @pl.when(relay_turn)
        def _():
            arrived(relay_in, relay_sem)
            start(*relay_copy())

            @pl.when(first)
            def _():
                arrived(relay_two, relay_two_sem)
                start(*relay_two_copy())

        for j in range(1, 4):
            to = (b + j) % 4
            rows = pl.ds(pl.multiple_of(32 * to, 32), 32)
            send(x_acc.at[:, rows, :], x_in.at[b], x_sem, device(ring, s, to // 2, to % 2))

        for e in range(2):
            main_out[e, 2] = far * y_acc[3 * e]
            to_owner(e, 2, 1)

        def edge_up():
            extra_out[0] = near * pairs[0] - far * pairs[1]
            start(extra_out.at[0], extra_in.at[s], extra_sem, device(ring + 1, 0, yo, co))

        def edge_down():
            extra_out[1] = far * pairs[2]
            start(extra_out.at[1], extra_in.at[s], extra_sem, device(ring - 1, 1, yo, co))

        def inner_y(e):
            main_out[e, 3] = far * y_acc[1 + e]
            to_owner(e, 3, 1)

        for q in groups(SAME_USE):
            arrived(late.at[q, pl.ds(2, 2)], edge_sem.at[q])
            arrived(late.at[q, 0], same_sem.at[q])
            pl.when(s == 0)(lambda: pair_sums(q, (2,)))
            pl.when(s == 1)(lambda: pair_sums(q, (0, 1)))
            y_current(late, q, s, 1 + s)
        pl.when(s == 0)(edge_down)
        pl.when(s == 1)(edge_up)
        pl.when(s == 0)(lambda: inner_y(0))
        pl.when(s == 1)(lambda: inner_y(1))

        for k, q in enumerate(order):
            arrived(late.at[q, 0], cross_sem.at[q])

            @pl.when(s == 1)
            def _():
                pair_sums(q, (2,))
                if k == 3:
                    edge_down()

            @pl.when((s == 0) & jnp.logical_not(ahead))
            def _():
                pair_sums(q, (0, 1))
                if k == 3:
                    edge_up()

            @pl.when((s == 0) & ahead)
            def _():
                pair_sums(q, (0, 1) if k < 2 else (1,))
                if k == 1:
                    pair_sums(order[2], (0,))
                    pair_sums(order[3], (0,))
                    pl.when(last)(edge_up)
                if k == 2:
                    pl.when(jnp.logical_not(last))(edge_up)

            pair_sums(q, range(3, 8))
            if k < 3:
                y_current(late, q, 1 - s, 2 - s)

        b1n0, b0n0, p1a1 = pairs[0], pairs[1], -pairs[2]
        a01, a1b0, b01, a0b0, a1b1 = -pairs[3], pairs[4], pairs[5], -pairs[6], pairs[7]
        main_out[0, 0] = near * a01 - far * a0b0
        main_out[0, 1] = near * (a1b0 + a01) - far * (a1b1 + p1a1)
        main_out[1, 0] = near * (b01 + a1b0) - far * (b0n0 + a0b0)
        main_out[1, 1] = near * (b1n0 + b01) - far * a1b1
        for e in range(2):
            to_owner(e, 0, 2)
        y_current(late, order[3], 1 - s, 2 - s)
        pl.when(s == 0)(lambda: inner_y(1))
        pl.when(s == 1)(lambda: inner_y(0))

        arrived(x_in.at[pl.ds(0, 3)], x_sem)
        total = x_acc[:, pl.ds(pl.multiple_of(32 * b, 32), 32), :]
        for j in range(1, 4):
            total = total + x_in[(b + j) % 4]
        out[1] = total * far
        def tip_current(q, tip, sem):
            arrived(tip, sem)

            def step(n, total):
                w = weights[q, pl.ds(n, 1), :]
                here = [w * outer[q, 0, n, p].astype(F32) for p in range(2)]
                there = [tip[n, p].astype(F32) for p in range(2)]
                return total + term(there, here)

            main_in[0, 0] -= far * lax.fori_loop(0, bands, step, jnp.zeros((16, 128), F32), unroll=8)

        pl.when(early & (s == 0))(lambda: tip_current(order[3], tip_in, tip_sem))
        pl.when(first & (s == 0))(lambda: tip_current(order[2], tip_two, tip_two_sem))
        pl.when(s == 0)(lambda: arrived(main_in.at[1], main_sem))
        pl.when(s == 1)(lambda: arrived(main_in, main_sem))
        for h in range(2):
            rows = slice(16 * h, 16 * h + 16)
            out[0, :, rows, :] = main_in[h, :2]
            out[2, s, rows, :] = main_in[h, 2]
            out[2, 1 - s, rows, :] = main_in[h, 3]

        def sent_copy(src, dst, sem, target):
            pltpu.make_async_remote_copy(
                src_ref=src, dst_ref=dst, send_sem=send_sem, recv_sem=sem, device_id=target, device_id_type=MESH
            ).wait_send()

        sent_copy(extra_out.at[0], extra_in.at[s], extra_sem, device(ring + 1, 0, yo, co))
        sent_copy(extra_out.at[1], extra_in.at[s], extra_sem, device(ring - 1, 1, yo, co))
        for part, size in ((0, 2), (2, 1), (3, 1)):
            sent_copy(*main_copy(1, part, size))

        @pl.when(s == 1)
        def _():
            for part, size in ((0, 2), (2, 1), (3, 1)):
                sent_copy(*main_copy(0, part, size))

        pl.when(tip_turn)(lambda: sent_copy(*tip_copy()))
        pl.when(relay_turn)(lambda: sent_copy(*relay_copy()))
        pl.when(tip_turn & last)(lambda: sent_copy(*tip_two_copy()))
        pl.when(relay_turn & first)(lambda: sent_copy(*relay_two_copy()))
        for copy in sent:
            copy.wait_send()

        arrived(extra_in, extra_sem)
        for h in range(2):
            out[0, s, 16 * h : 16 * h + 16, :] += extra_in[h]

    return kernel


def solution(mesh):
    rings = mesh.shape["grid"] // 2

    def per_device(orbitals, occupations):
        n = orbitals.shape[0]
        dma = pltpu.SemaphoreType.DMA
        chunk = (n, 2, 16, 128)
        return pl.pallas_call(
            make_kernel(rings),
            out_shape=pltpu.VMEM((3, 2, 32, 128), F32),
            in_specs=[pl.BlockSpec(memory_space=pl.ANY), pl.BlockSpec(memory_space=pl.ANY)],
            out_specs=pl.BlockSpec(memory_space=pltpu.VMEM),
            scratch_shapes=[
                pltpu.SMEM((n,), F32),
                pltpu.VMEM((n, 2, 2, 128, 128), BF16),
                pltpu.VMEM((4, 2, *chunk), BF16),
                pltpu.VMEM((4, 4, *chunk), BF16),
                pltpu.VMEM((4, n, 128), F32),
                pltpu.VMEM((128, 128), BF16),
                pltpu.VMEM((128, 128), BF16),
                pltpu.VMEM((2, 128, 128), F32),
                pltpu.VMEM((4, 2, 32, 128), F32),
                pltpu.VMEM((4, 16, 128), F32),
                pltpu.VMEM((8, 16, 128), F32),
                pltpu.VMEM((2, 4, 16, 128), F32),
                pltpu.VMEM((2, 4, 16, 128), F32),
                pltpu.VMEM((2, 16, 128), F32),
                pltpu.VMEM((2, 16, 128), F32),
                pltpu.VMEM(chunk, BF16),
                pltpu.VMEM(chunk, BF16),
                pltpu.VMEM(chunk, BF16),
                pltpu.VMEM(chunk, BF16),
                dma, dma((3,)), dma, dma((4,)), dma((4,)), dma((4,)), dma((4,)), dma, dma, dma, dma, dma, dma, dma, dma,
                pltpu.SemaphoreType.REGULAR, pltpu.SemaphoreType.REGULAR,
            ],
            compiler_params=pltpu.CompilerParams(collective_id=0, has_side_effects=True),
        )(orbitals, occupations)

    return jax.shard_map(
        per_device,
        mesh=mesh,
        in_specs=(P("band", None, "grid", None, None), P("band")),
        out_specs=P(None, "grid", "band", None),
        check_vma=False,
    )
```
